32 devices in a mesh: seq: 2 (over x), mp: 4 (over y, core), dp: 4 (over z).
Axes of the slice: x: 2, y: 2, z: 4, core: 2. Of those that a mesh axis runs over, the one named last changes fastest.
Arguments:
- tokens: bfloat16 [16384, 2048], P(('dp', 'seq'), 'mp'), parts along dimension 0, may hold values from -6 to 6
- w_query: bfloat16 [2048, 2048], P(None, 'mp'), may hold values from -0.125 to 0.125
- w_key: bfloat16 [2048, 2048], P(None, 'mp'), may hold values from -0.125 to 0.125
- w_value: bfloat16 [2048, 2048], P(None, 'mp'), may hold values from -0.125 to 0.125
- w_gate: bfloat16 [2048, 2048], P(None, 'mp'), may hold values from -0.125 to 0.125
- decay_exponent: int32 [16], P('mp'), may hold values from 5 to 16
- forget: float32 [16384, 16], P(('dp', 'seq'), 'mp'), parts along dimension 0, may hold values from 0 to 0.69
- norm_gain: float32 [2048], replicated, may hold values from 0.1 to 1.9
Outputs:
- retained: bfloat16 [16384, 2048], P(('dp', 'seq', 'mp')), parts along dimension 0
The draws below stay inside these ranges and needn't reach their ends.
There are 4 independent parts, one for each index of `dp`. The reference program is written for one: setup_inputs(seed, part) draws one part's arguments, and reference() takes and returns one part's arrays. A program takes and returns all parts, laid end to end along the dimension named above; an argument that names none is the same for every part. Nothing has to cross between parts.
All inputs are finite; a program needn't handle non-finite values.
Results may differ from the reference program's by a relative error of at most 0.015.
Values may be sent and summed in bfloat16 or wider, within the bound.
A program may use at most 64 MiB of HBM per device.

```python
import jax
import jax.numpy as jnp
from jax import lax

D = 2048
HEADS = 16
DH = 128
TOKENS = 4096
FEATURES = 2048


def draw_forget(key, part):
    first_key, second_key = jax.random.split(jax.random.fold_in(key, 11))
    chance = jax.random.uniform(first_key, (TOKENS, HEADS), jnp.float32)
    amount = jax.random.uniform(second_key, (TOKENS, HEADS), jnp.float32, 0.22, 0.69)
    return jnp.where(chance < 6.0 / TOKENS, amount, 0.0).astype(jnp.float32)


def with_ends(entries, key, low, high):
    spot = [jax.random.randint(jax.random.fold_in(key, axis), (), 0, length) for axis, length in enumerate(entries.shape)]
    longest = entries.shape.index(max(entries.shape))
    next_to = spot[:longest] + [(spot[longest] + 1) % entries.shape[longest]] + spot[longest + 1:]
    return entries.at[tuple(spot)].set(low).at[tuple(next_to)].set(high)


def level_of(rng, extent, shards, smallest, top_value):
    level, own = 1.0, jax.random.fold_in(rng, 6)
    for axis_at, shards_of in shards:
        heights = jnp.exp(jax.random.uniform(jax.random.fold_in(own, axis_at), (shards_of,), jnp.float32, smallest / len(shards), top_value / len(shards)))
        level = level * jnp.repeat(heights, extent[axis_at] // shards_of).reshape([-1 if axis == axis_at else 1 for axis in range(len(extent))])
    return level


def normal_values(key, extent, spread, reach, shards=(), kind=jnp.bfloat16):
    level = level_of(key, extent, shards, -0.22, 0.18) if shards else 1.0
    values = jax.random.normal(key, extent, jnp.float32) * spread * level
    return jnp.minimum(jnp.maximum(values, -reach), reach).astype(kind)


def setup_inputs(seed: int = 0, part: int = 0) -> dict:
    keys = jax.random.split(jax.random.key(seed), 9)
    part_splits = jax.random.split(jax.random.fold_in(keys[8], part), 9)
    return {
        "tokens": normal_values(part_splits[0], (TOKENS, D), 1.0, 6.0, ((0, 2), (1, 4))),
        "w_query": normal_values(keys[1], (D, FEATURES), D ** -0.5, 0.125, ((1, 4),)),
        "w_key": normal_values(keys[2], (D, FEATURES), D ** -0.5, 0.125, ((1, 4),)),
        "w_value": normal_values(keys[3], (D, FEATURES), D ** -0.5, 0.125, ((1, 4),)),
        "w_gate": normal_values(keys[4], (D, FEATURES), D ** -0.5, 0.125, ((1, 4),)),
        "decay_exponent": with_ends(jax.random.randint(keys[5], (HEADS,), 5, 17), jax.random.fold_in(keys[5], 1), 5, 16).astype(jnp.int32),
        "forget": draw_forget(jax.random.fold_in(jax.random.fold_in(keys[8], part), 71), part),
        "norm_gain": jnp.clip(1.0 + 0.18 * jax.random.normal(keys[7], (FEATURES,), jnp.float32), 0.1, 1.9),
    }


def retention(queries, key_rows, values, logdecay):
    seq_rows = queries.shape[0]
    head_count = logdecay.shape[1]
    head_width = queries.shape[1] // head_count
    block_rows = 512 if seq_rows % 512 == 0 else seq_rows
    block_count = seq_rows // block_rows

    def shaped(source):
        return source.reshape(block_count, block_rows, head_count, head_width)
    decays = logdecay.reshape(block_count, block_rows, head_count)
    position = lax.broadcasted_iota(jnp.int32, (block_rows, block_rows), 0)
    earlier = lax.broadcasted_iota(jnp.int32, (block_rows, block_rows), 1)
    causal = position >= earlier

    def advance(kv_state, pieces):
        query_blk, key_blk, value_blk, decay_blk = pieces
        running = jnp.cumsum(decay_blk, axis=0)
        heads_first = running.T
        log_gap = heads_first[:, :, None] - heads_first[:, None, :]
        decay_mask = jnp.where(causal[None], jnp.exp(jnp.where(causal[None], log_gap, 0.0)), 0.0)
        query_float = query_blk.astype(jnp.float32)
        key_float = key_blk.astype(jnp.float32)
        value_float = value_blk.astype(jnp.float32)
        scores = (jnp.einsum('tha,sha->hts', query_float, key_float) * decay_mask).astype(jnp.bfloat16)
        inner = jnp.einsum('hts,shb->thb', scores.astype(jnp.float32), value_float)
        carried = jnp.einsum('tha,hab->thb', query_float * jnp.exp(running)[:, :, None], kv_state, precision=lax.Precision.HIGHEST)
        key_scaled = key_float * jnp.exp(running[-1:] - running)[:, :, None]
        kv_state = jnp.exp(running[-1])[:, None, None] * kv_state + jnp.einsum('sha,shb->hab', key_scaled, value_float, precision=lax.Precision.HIGHEST)
        return (kv_state, (inner + carried).astype(jnp.bfloat16))
    initial = jnp.zeros((head_count, head_width, head_width), jnp.float32)
    final_state, outputs = lax.scan(advance, initial, (shaped(queries), shaped(key_rows), shaped(values), decays))
    return outputs.reshape(seq_rows, head_count * head_width)

def reference(tokens, w_query, w_key, w_value, w_gate, decay_exponent, forget, norm_gain):
    queries = jnp.dot(tokens, w_query, preferred_element_type=jnp.float32).astype(jnp.bfloat16)
    key_rows = (jnp.dot(tokens, w_key, preferred_element_type=jnp.float32) * DH ** (-0.5)).astype(jnp.bfloat16)
    values = jnp.dot(tokens, w_value, preferred_element_type=jnp.float32).astype(jnp.bfloat16)
    gate = jnp.dot(tokens, w_gate, preferred_element_type=jnp.float32).astype(jnp.bfloat16)
    rate = jnp.log1p(-jnp.exp2(-decay_exponent.astype(jnp.float32)))
    logdecay = rate[None, :] - forget
    output = retention(queries, key_rows, values, logdecay).astype(jnp.float32)
    squares = lax.optimization_barrier(jnp.mean(output * output, axis=1))
    rstd = lax.rsqrt(squares + 1e-06)
    gated = jax.nn.silu(gate.astype(jnp.float32)) * output * rstd[:, None] * norm_gain[None, :]
    return gated.astype(jnp.bfloat16)
```

```python
import functools

import jax
import jax.numpy as jnp
from jax import lax
from jax.experimental import pallas as pl
from jax.experimental.pallas import tpu as pltpu
from jax.sharding import PartitionSpec as P

DH = 128
MESH = pl.DeviceIdType.MESH
F32 = jnp.float32
BF16 = jnp.bfloat16


def contract(a, b, dims):
    return lax.dot_general(a, b, ((dims[0], dims[1]), ((), ())), preferred_element_type=F32)


def kernel(
    n_mp, n_seq, heads, rows, groups,
    tokens, wq, wk, wv, wg, exponent_in, forget_in, gain_in, out,
    x, w, exponent, forget, gain, partial, local_out, q_in, gates, moved, got, sq_out, sq_got,
    state, held, enter, state_out, state_got, offset,
    weight_sem, small_sem, own_sem, y_send, y_recv, d_send, d_recv, s_send, s_recv, m_send, m_recv, q_send, q_recv,
):
    me = lax.axis_index("mp")
    place = lax.axis_index("seq")
    chips = n_mp // 2
    chip, core = me // 2, me % 2
    partner = chip * 2 + (1 - core)
    seq_rows, width = tokens.shape
    chunks = seq_rows // rows
    own_rows = seq_rows // n_mp
    parts = own_rows // rows
    head_width = width // heads
    group_heads = heads // groups
    group_width = width // groups

    barrier = pltpu.get_barrier_semaphore()
    for other in range(1, n_mp):
        pl.semaphore_signal(barrier, inc=1, device_id={"mp": lax.rem(me + other, n_mp)}, device_id_type=MESH)

    @pl.when(place > 0)
    def _():
        pl.semaphore_signal(barrier, inc=1, device_id={"seq": place - 1}, device_id_type=MESH)

    @pl.when(place < n_seq - 1)
    def _():
        pl.semaphore_signal(barrier, inc=1, device_id={"seq": place + 1}, device_id_type=MESH)

    weights = [pltpu.make_async_copy(src, w.at[i], weight_sem.at[i]) for i, src in enumerate((wk, wv, wq, wg))]
    small = [
        pltpu.make_async_copy(src, dst, small_sem.at[i])
        for i, (src, dst) in enumerate(((exponent_in, exponent), (forget_in, forget), (gain_in, gain)))
    ]

    def columns(block):
        return pl.ds(pl.multiple_of(block * width, width), width)

    def at_rows(c):
        return pl.ds(pl.multiple_of(c * rows, rows), rows)

    def own_copy(c):
        return pltpu.make_async_copy(tokens.at[at_rows(c), :], x.at[at_rows(c), columns(me)], own_sem.at[c])

    def far(step):
        return lax.rem(chip + step, chips) * 2 + core

    def back(step):
        return lax.rem(chip + chips - step, chips) * 2 + core

    def back_other(step):
        return lax.rem(chip + chips - step, chips) * 2 + (1 - core)

    def y_copy(c, step):
        return pltpu.make_async_remote_copy(
            src_ref=tokens.at[at_rows(c), :], dst_ref=x.at[at_rows(c), columns(me)],
            send_sem=y_send.at[c, step], recv_sem=y_recv.at[c, step],
            device_id={"mp": far(step)}, device_id_type=MESH)

    def y_arrival(c, step):
        return pltpu.make_async_remote_copy(
            src_ref=tokens.at[at_rows(c), :], dst_ref=x.at[at_rows(c), columns(back(step))],
            send_sem=y_send.at[c, step], recv_sem=y_recv.at[c, step],
            device_id={"mp": far(step)}, device_id_type=MESH)

    def d_copy(c, step):
        block = me if step == 0 else back(step)
        source = tokens.at[at_rows(c), :] if step == 0 else x.at[at_rows(c), columns(block)]
        return pltpu.make_async_remote_copy(
            src_ref=source, dst_ref=x.at[at_rows(c), columns(block)],
            send_sem=d_send.at[c, step], recv_sem=d_recv.at[c, step],
            device_id={"mp": partner}, device_id_type=MESH)

    def d_arrival(c, step):
        there = x.at[at_rows(c), columns(partner if step == 0 else back_other(step))]
        return pltpu.make_async_remote_copy(
            src_ref=there, dst_ref=there, send_sem=d_send.at[c, step], recv_sem=d_recv.at[c, step],
            device_id={"mp": partner}, device_id_type=MESH)

    for copy in small:
        copy.start()
    own_copy(0).start()
    for copy in weights:
        copy.start()
    pl.loop(1, chunks)(lambda c: own_copy(c).start())

    neighbours = jnp.minimum(place, 1) + jnp.minimum(n_seq - 1 - place, 1)
    pl.semaphore_wait(barrier, n_mp - 1 + neighbours)

    @pl.loop(0, chunks)
    def _(c):
        for step in range(1, chips):
            y_copy(c, step).start()
        d_copy(c, 0).start()

    state[...] = jnp.zeros_like(state)
    offset[...] = jnp.zeros_like(offset)
    enter[...] = jnp.zeros_like(enter)

    later = lax.broadcasted_iota(jnp.int32, (rows, rows), 0)
    earlier = lax.broadcasted_iota(jnp.int32, (rows, rows), 1)
    causal = later >= earlier
    summing = (later <= earlier).astype(F32)
    exact = lax.Precision.HIGHEST
    ones = jnp.ones((8, head_width), BF16)

    for copy in small:
        copy.wait()
    spread = jnp.broadcast_to(exponent[...].astype(F32), (heads, heads))
    diagonal = lax.broadcasted_iota(jnp.int32, (heads, heads), 0) == lax.broadcasted_iota(jnp.int32, (heads, heads), 1)
    column = jnp.sum(jnp.where(diagonal, spread, 0.0), axis=1, keepdims=True)
    rate = jnp.log1p(-jnp.exp2(-column))
    for copy in weights:
        copy.wait()

    def s_copy(g):
        part = pl.ds(g * group_heads, group_heads)
        return pltpu.make_async_remote_copy(
            src_ref=state_out.at[part], dst_ref=state_got.at[part], send_sem=s_send.at[g], recv_sem=s_recv.at[g],
            device_id={"seq": lax.rem(place + 1, n_seq)}, device_id_type=MESH)

    def group_columns(g):
        return pl.ds(g * group_width, group_width)

    def m_copy(block, g):
        to, r = block // parts, lax.rem(block, parts)
        return pltpu.make_async_remote_copy(
            src_ref=moved.at[at_rows(block), group_columns(g)], dst_ref=got.at[me, at_rows(r), group_columns(g)],
            send_sem=m_send.at[block, g], recv_sem=m_recv.at[me, r, g],
            device_id={"mp": to}, device_id_type=MESH)

    def q_copy(block):
        to, r = block // parts, lax.rem(block, parts)
        return pltpu.make_async_remote_copy(
            src_ref=sq_out.at[block], dst_ref=sq_got.at[me, r],
            send_sem=q_send.at[block], recv_sem=q_recv.at[me, r],
            device_id={"mp": to}, device_id_type=MESH)

    def finalize(block, g):
        here = at_rows(block)
        to, r = block // parts, lax.rem(block, parts)
        squares = jnp.zeros((8, rows), F32)
        for h in range(g * group_heads, (g + 1) * group_heads):
            part = slice(h * head_width, (h + 1) * head_width)
            whole = local_out[here, part] + jnp.dot(q_in[here, part], enter[h], preferred_element_type=F32)
            kept = whole.astype(BF16).astype(F32)
            moved[here, part] = (gates[here, part] * kept).astype(BF16)
            square = kept * kept
            high = square.astype(BF16)
            low = (square - high.astype(F32)).astype(BF16)
            squares += contract(ones, high, ((1,), (1,))) + contract(ones, low, ((1,), (1,)))
        total = squares[0:1, :]
        if g > 0:
            total = total + sq_out[block]
        sq_out[block] = total

        @pl.when(to != me)
        def _():
            if g == groups - 1:
                q_copy(block).start()
            m_copy(block, g).start()

        @pl.when(to == me)
        def _():
            part = slice(g * group_width, (g + 1) * group_width)
            got[me, at_rows(r), part] = moved[here, part]
            if g == groups - 1:
                sq_got[me, r] = total

    @pl.loop(0, chunks)
    def _(c):
        here = at_rows(c)
        decay = rate - forget[:, here]
        running = jnp.dot(decay, summing, precision=exact, preferred_element_type=F32)
        by_row = lax.dot_general(
            causal.astype(F32), decay, (((1,), (1,)), ((), ())), precision=exact, preferred_element_type=F32)
        last = running[:, rows - 1 :]
        before = offset[...]

        own_copy(c).wait()
        d_arrival(c, 0).wait_recv()
        own_side = pl.ds(pl.multiple_of(chip * 2 * width, 2 * width), 2 * width)
        piece = x[here, own_side]
        for i in range(4):
            partial[i] = jnp.dot(piece, w[i, own_side, :], preferred_element_type=F32)
        for step in range(1, chips):
            y_arrival(c, step).wait_recv()
            d_copy(c, step).start()
        for step in range(1, chips):
            piece = x[here, columns(back(step))]
            for i in range(4):
                partial[i] += jnp.dot(piece, w[i, columns(back(step)), :], preferred_element_type=F32)
        for step in range(1, chips):
            d_arrival(c, step).wait_recv()

        def project(i):
            total = partial[i]
            for step in range(1, chips):
                total += jnp.dot(
                    x[here, columns(back_other(step))], w[i, columns(back_other(step)), :],
                    preferred_element_type=F32)
            return total

        key = (project(0) * DH ** (-0.5)).astype(BF16)
        value = project(1).astype(BF16)
        for h in range(heads):
            part = slice(h * head_width, (h + 1) * head_width)
            k, v = key[:, part], value[:, part]
            end = last[h : h + 1, :]
            grown = state[h]
            held[h] = grown.astype(BF16)
            faded = (k.astype(F32) * jnp.exp(end - by_row[:, h : h + 1])).astype(BF16)
            state[h] = jnp.exp(end) * grown + contract(faded, v, ((0,), (0,)))

        @pl.when(jnp.logical_and(place == 0, c == chunks - 1))
        def _():
            state_out[...] = state[...].astype(BF16)
            if n_seq > 1:
                for g in range(groups):
                    s_copy(g).start()

        query = project(2).astype(BF16)
        for h in range(heads):
            part = slice(h * head_width, (h + 1) * head_width)
            q, k, v = query[:, part], key[:, part], value[:, part]
            col = by_row[:, h : h + 1]
            mask = jnp.exp(jnp.where(causal, col - running[h : h + 1, :], -1e30))
            scores = (contract(q, k, ((1,), (1,))) * mask).astype(BF16)
            qf = q.astype(F32)
            carried = jnp.dot((qf * jnp.exp(col)).astype(BF16), held[h], preferred_element_type=F32)
            local_out[here, part] = jnp.dot(scores, v, preferred_element_type=F32) + carried
            q_in[here, part] = (qf * jnp.exp(col + before[h : h + 1, 0:1])).astype(BF16)
        offset[...] = before + last
        gate = project(3).astype(BF16).astype(F32)
        gates[here, :] = gate / (1.0 + jnp.exp(-gate))

        @pl.when(place == 0)
        def _():
            for g in range(groups):
                finalize(c, g)

    far_steps = (n_mp - 2) * parts

    def in_order(step):
        o = lax.rem(step, n_mp - 2)
        away = (lax.rem(chip + o // 2 + 1, chips) * 2 + lax.rem(core + o, 2)) * parts + step // (n_mp - 2)
        rest = jnp.maximum(step - far_steps, 0)
        home = (chip * 2 + lax.rem(core + 1 + rest, 2)) * parts + rest // 2
        return jnp.where(step < far_steps, away, home)

    if n_seq > 1:
        @pl.when(place > 0)
        def _():
            for g in range(groups):
                part = slice(g * group_heads, (g + 1) * group_heads)
                s_copy(g).wait_recv()
                enter[part] = state_got[part]
                if n_seq > 2:
                    @pl.when(place < n_seq - 1)
                    def _():
                        for h in range(g * group_heads, (g + 1) * group_heads):
                            total = jnp.exp(offset[h : h + 1, 0:1])
                            state_out[h] = (total * enter[h].astype(F32) + state[h]).astype(BF16)
                        s_copy(g).start()

                pl.loop(0, chunks)(lambda step: finalize(in_order(step), g))

    def m_arrival(source, r, g):
        there = got.at[source, at_rows(r), group_columns(g)]
        return pltpu.make_async_remote_copy(
            src_ref=there, dst_ref=there, send_sem=m_send.at[0, 0], recv_sem=m_recv.at[source, r, g],
            device_id={"mp": partner}, device_id_type=MESH)

    def q_arrival(source, r):
        there = sq_got.at[source, r]
        return pltpu.make_async_remote_copy(
            src_ref=there, dst_ref=there, send_sem=q_send.at[0], recv_sem=q_recv.at[source, r],
            device_id={"mp": partner}, device_id_type=MESH)

    sources = [me, partner] + [lax.rem(chip + t, chips) * 2 + lax.rem(core + s, 2) for t in range(1, chips) for s in (0, 1)]

    for r in range(parts):
        for source in sources[1:]:
            q_arrival(source, r).wait_recv()
        total = sq_got[0, r]
        for source in range(1, n_mp):
            total += sq_got[source, r]
        scale = lax.rsqrt(total * (1.0 / (n_mp * width)) + 1e-06)
        scale = jnp.broadcast_to(scale, (8, rows)).T[:, 0:1]
        span = slice(r * rows, (r + 1) * rows)
        for g in range(groups):
            for i, source in enumerate(sources):
                if i > 0:
                    m_arrival(source, r, g).wait_recv()
                part = pl.ds(pl.multiple_of(source * width + g * group_width, group_width), group_width)
                piece = got[source, span, g * group_width : (g + 1) * group_width].astype(F32)
                out[span, part] = (piece * scale * gain[:, part]).astype(BF16)

    @pl.loop(0, chunks)
    def _(c):
        for step in range(1, chips):
            y_copy(c, step).wait_send()
        for step in range(chips):
            d_copy(c, step).wait_send()

        @pl.when(c // parts != me)
        def _():
            q_copy(c).wait_send()
            for g in range(groups):
                m_copy(c, g).wait_send()

    if n_seq > 1:
        @pl.when(place < n_seq - 1)
        def _():
            for g in range(groups):
                s_copy(g).wait_send()


def body(n_mp, n_seq, tokens, w_query, w_key, w_value, w_gate, decay_exponent, forget, norm_gain):
    seq_rows, width = tokens.shape
    features = w_query.shape[0]
    heads = decay_exponent.shape[0]
    own_rows = seq_rows // n_mp
    rows = 256 if own_rows % 256 == 0 else own_rows
    chunks, parts = seq_rows // rows, own_rows // rows
    groups = 2 if heads % 2 == 0 else 1
    hbm = pl.BlockSpec(memory_space=pl.ANY)
    dma = pltpu.SemaphoreType.DMA
    chips = n_mp // 2
    return pl.pallas_call(
        functools.partial(kernel, n_mp, n_seq, heads, rows, groups),
        out_shape=pltpu.VMEM((own_rows, features), BF16),
        in_specs=[hbm] * 8,
        out_specs=pl.BlockSpec(memory_space=pltpu.VMEM),
        scratch_shapes=[
            pltpu.VMEM((seq_rows, features), BF16),
            pltpu.VMEM((4, features, width), BF16),
            pltpu.VMEM((1, heads), jnp.int32),
            pltpu.VMEM((heads, seq_rows), F32),
            pltpu.VMEM((1, features), F32),
            pltpu.VMEM((4, rows, width), F32),
            pltpu.VMEM((seq_rows, width), F32),
            pltpu.VMEM((seq_rows, width), BF16),
            pltpu.VMEM((seq_rows, width), F32),
            pltpu.VMEM((seq_rows, width), BF16),
            pltpu.VMEM((n_mp, own_rows, width), BF16),
            pltpu.VMEM((chunks, 1, rows), F32),
            pltpu.VMEM((n_mp, parts, 1, rows), F32),
            pltpu.VMEM((heads, DH, DH), F32),
            pltpu.VMEM((heads, DH, DH), BF16),
            pltpu.VMEM((heads, DH, DH), BF16),
            pltpu.VMEM((heads, DH, DH), BF16),
            pltpu.VMEM((heads, DH, DH), BF16),
            pltpu.VMEM((heads, 128), F32),
            dma((4,)),
            dma((3,)),
            dma((chunks,)),
            dma((chunks, chips)),
            dma((chunks, chips)),
            dma((chunks, chips)),
            dma((chunks, chips)),
            dma((groups,)),
            dma((groups,)),
            dma((chunks, groups)),
            dma((n_mp, parts, groups)),
            dma((chunks,)),
            dma((n_mp, parts)),
        ],
        compiler_params=pltpu.CompilerParams(
            collective_id=0, has_side_effects=True, vmem_limit_bytes=48 * 1024 * 1024
        ),
    )(tokens, w_query, w_key, w_value, w_gate, decay_exponent[None, :], forget.T, norm_gain[None, :])


def solution(mesh):
    placed = (
        P(("dp", "seq"), "mp"),
        P(None, "mp"),
        P(None, "mp"),
        P(None, "mp"),
        P(None, "mp"),
        P("mp"),
        P(("dp", "seq"), "mp"),
        P(),
    )
    return jax.shard_map(
        functools.partial(body, mesh.shape["mp"], mesh.shape["seq"]),
        mesh=mesh,
        in_specs=placed,
        out_specs=P(("dp", "seq", "mp"), None),
        check_vma=False,
    )
```

```python
import functools

import jax
import jax.numpy as jnp
from jax import lax
from jax.experimental import pallas as pl
from jax.experimental.pallas import tpu as pltpu
from jax.sharding import PartitionSpec as P

DH = 128
MESH = pl.DeviceIdType.MESH
F32 = jnp.float32
BF16 = jnp.bfloat16


def contract(a, b, dims):
    return lax.dot_general(a, b, ((dims[0], dims[1]), ((), ())), preferred_element_type=F32)


def kernel(
    n_mp, n_seq, heads, rows, groups,
    tokens, wq, wk, wv, wg, exponent_in, forget_in, gain_in, out,
    x, w, exponent, forget, gain, partial, local_out, q_in, gates, moved, got, sq_out, sq_got,
    state, held, enter, state_out, state_got, offset, hop_in, hop_out,
    weight_sem, small_sem, own_sem, y_send, y_recv, d_send, d_recv, s_send, s_recv, m_send, m_recv, q_send, q_recv, hop_send, hop_recv,
):
    me = lax.axis_index("mp")
    place = lax.axis_index("seq")
    chips = n_mp // 2
    chip, core = me // 2, me % 2
    partner = chip * 2 + (1 - core)
    seq_rows, width = tokens.shape
    chunks = seq_rows // rows
    own_rows = seq_rows // n_mp
    parts = own_rows // rows
    head_width = width // heads
    group_heads = heads // groups
    group_width = width // groups
    relay = n_seq == 2 and chips == 2
    hop_rows = hop_in.shape[0]
    tail_rows = pl.ds(seq_rows - hop_rows, hop_rows)
    head_rows = pl.ds(seq_rows - rows, rows - hop_rows)
    across = lax.rem(chip + 1, chips) * 2 + core

    barrier = pltpu.get_barrier_semaphore()
    for other in range(1, n_mp):
        pl.semaphore_signal(barrier, inc=1, device_id={"mp": lax.rem(me + other, n_mp)}, device_id_type=MESH)

    @pl.when(place > 0)
    def _():
        pl.semaphore_signal(barrier, inc=1, device_id={"seq": place - 1}, device_id_type=MESH)

    @pl.when(place < n_seq - 1)
    def _():
        pl.semaphore_signal(barrier, inc=1, device_id={"seq": place + 1}, device_id_type=MESH)

    if relay:
        pl.semaphore_signal(barrier, inc=1, device_id={"mp": across, "seq": 1 - place}, device_id_type=MESH)

    weights = [pltpu.make_async_copy(src, w.at[i], weight_sem.at[i]) for i, src in enumerate((wk, wv, wq, wg))]
    small = [
        pltpu.make_async_copy(src, dst, small_sem.at[i])
        for i, (src, dst) in enumerate(((exponent_in, exponent), (forget_in, forget), (gain_in, gain)))
    ]

    def columns(block):
        return pl.ds(pl.multiple_of(block * width, width), width)

    def at_rows(c):
        return pl.ds(pl.multiple_of(c * rows, rows), rows)

    def own_copy(c):
        return pltpu.make_async_copy(tokens.at[at_rows(c), :], x.at[at_rows(c), columns(me)], own_sem.at[c])

    def far(step):
        return lax.rem(chip + step, chips) * 2 + core

    def back(step):
        return lax.rem(chip + chips - step, chips) * 2 + core

    def back_other(step):
        return lax.rem(chip + chips - step, chips) * 2 + (1 - core)

    def y_copy(c, step):
        return pltpu.make_async_remote_copy(
            src_ref=tokens.at[at_rows(c), :], dst_ref=x.at[at_rows(c), columns(me)],
            send_sem=y_send.at[c, step], recv_sem=y_recv.at[c, step],
            device_id={"mp": far(step)}, device_id_type=MESH)

    def y_arrival(c, step):
        return pltpu.make_async_remote_copy(
            src_ref=tokens.at[at_rows(c), :], dst_ref=x.at[at_rows(c), columns(back(step))],
            send_sem=y_send.at[c, step], recv_sem=y_recv.at[c, step],
            device_id={"mp": far(step)}, device_id_type=MESH)

    def d_copy(c, step):
        block = me if step == 0 else back(step)
        source = tokens.at[at_rows(c), :] if step == 0 else x.at[at_rows(c), columns(block)]
        return pltpu.make_async_remote_copy(
            src_ref=source, dst_ref=x.at[at_rows(c), columns(block)],
            send_sem=d_send.at[c, step], recv_sem=d_recv.at[c, step],
            device_id={"mp": partner}, device_id_type=MESH)

    def d_arrival(c, step):
        there = x.at[at_rows(c), columns(partner if step == 0 else back_other(step))]
        return pltpu.make_async_remote_copy(
            src_ref=there, dst_ref=there, send_sem=d_send.at[c, step], recv_sem=d_recv.at[c, step],
            device_id={"mp": partner}, device_id_type=MESH)

    def hop_copy(i):
        if i == 0:
            source, there, to = tokens.at[tail_rows, :], hop_in, {"mp": across, "seq": 1}
        elif i == 1:
            source, there, to = hop_in, x.at[tail_rows, columns(across)], {"seq": 0}
        else:
            source, there, to = hop_out, got.at[across, at_rows(0), pl.ds(0, group_width)], {"seq": 1}
        arrival = (hop_recv.at[0], y_recv.at[chunks - 1, 1], m_recv.at[across, 0, 0])[i]
        return pltpu.make_async_remote_copy(
            src_ref=source, dst_ref=there, send_sem=hop_send.at[i], recv_sem=arrival,
            device_id=to, device_id_type=MESH)

    def y_short():
        return pltpu.make_async_remote_copy(
            src_ref=tokens.at[head_rows, :], dst_ref=x.at[head_rows, columns(me)],
            send_sem=y_send.at[chunks - 1, 1], recv_sem=y_recv.at[chunks - 1, 1],
            device_id={"mp": across}, device_id_type=MESH)

    def out_hop(block):
        return pltpu.make_async_remote_copy(
            src_ref=moved.at[at_rows(block), pl.ds(0, group_width)], dst_ref=hop_out,
            send_sem=m_send.at[block, 0], recv_sem=hop_recv.at[1],
            device_id={"mp": across, "seq": 0}, device_id_type=MESH)

    for copy in small:
        copy.start()
    own_copy(0).start()
    for copy in weights:
        copy.start()
    pl.loop(1, chunks)(lambda c: own_copy(c).start())

    neighbours = jnp.minimum(place, 1) + jnp.minimum(n_seq - 1 - place, 1)
    pl.semaphore_wait(barrier, n_mp - 1 + neighbours + (1 if relay else 0))

    if relay:
        @pl.when(place == 0)
        def _():
            hop_copy(0).start()

    @pl.loop(0, chunks - 1 if relay else chunks)
    def _(c):
        for step in range(1, chips):
            y_copy(c, step).start()
        d_copy(c, 0).start()

    if relay:
        @pl.when(place == 0)
        def _():
            y_short().start()

        @pl.when(place == 1)
        def _():
            y_copy(chunks - 1, 1).start()

        d_copy(chunks - 1, 0).start()

    state[...] = jnp.zeros_like(state)
    offset[...] = jnp.zeros_like(offset)
    enter[...] = jnp.zeros_like(enter)

    later = lax.broadcasted_iota(jnp.int32, (rows, rows), 0)
    earlier = lax.broadcasted_iota(jnp.int32, (rows, rows), 1)
    causal = later >= earlier
    summing = (later <= earlier).astype(F32)
    exact = lax.Precision.HIGHEST
    ones = jnp.ones((8, head_width), BF16)

    for copy in small:
        copy.wait()
    spread = jnp.broadcast_to(exponent[...].astype(F32), (heads, heads))
    diagonal = lax.broadcasted_iota(jnp.int32, (heads, heads), 0) == lax.broadcasted_iota(jnp.int32, (heads, heads), 1)
    column = jnp.sum(jnp.where(diagonal, spread, 0.0), axis=1, keepdims=True)
    rate = jnp.log1p(-jnp.exp2(-column))
    for copy in weights:
        copy.wait()

    def s_copy(g):
        part = pl.ds(g * group_heads, group_heads)
        return pltpu.make_async_remote_copy(
            src_ref=state_out.at[part], dst_ref=state_got.at[part], send_sem=s_send.at[g], recv_sem=s_recv.at[g],
            device_id={"seq": lax.rem(place + 1, n_seq)}, device_id_type=MESH)

    def group_columns(g):
        return pl.ds(g * group_width, group_width)

    def m_copy(block, g):
        to, r = block // parts, lax.rem(block, parts)
        return pltpu.make_async_remote_copy(
            src_ref=moved.at[at_rows(block), group_columns(g)], dst_ref=got.at[me, at_rows(r), group_columns(g)],
            send_sem=m_send.at[block, g], recv_sem=m_recv.at[me, r, g],
            device_id={"mp": to}, device_id_type=MESH)

    def q_copy(block):
        to, r = block // parts, lax.rem(block, parts)
        return pltpu.make_async_remote_copy(
            src_ref=sq_out.at[block], dst_ref=sq_got.at[me, r],
            send_sem=q_send.at[block], recv_sem=q_recv.at[me, r],
            device_id={"mp": to}, device_id_type=MESH)

    def finalize(block, g, detour=False):
        here = at_rows(block)
        to, r = block // parts, lax.rem(block, parts)
        squares = jnp.zeros((8, rows), F32)
        for h in range(g * group_heads, (g + 1) * group_heads):
            part = slice(h * head_width, (h + 1) * head_width)
            whole = local_out[here, part] + jnp.dot(q_in[here, part], enter[h], preferred_element_type=F32)
            kept = whole.astype(BF16).astype(F32)
            moved[here, part] = (gates[here, part] * kept).astype(BF16)
            square = kept * kept
            high = square.astype(BF16)
            low = (square - high.astype(F32)).astype(BF16)
            squares += contract(ones, high, ((1,), (1,))) + contract(ones, low, ((1,), (1,)))
        total = squares[0:1, :]
        if g > 0:
            total = total + sq_out[block]
        sq_out[block] = total

        @pl.when(to != me)
        def _():
            if g == groups - 1:
                q_copy(block).start()
            (out_hop(block) if detour else m_copy(block, g)).start()

        @pl.when(to == me)
        def _():
            part = slice(g * group_width, (g + 1) * group_width)
            got[me, at_rows(r), part] = moved[here, part]
            if g == groups - 1:
                sq_got[me, r] = total

    @pl.loop(0, chunks)
    def _(c):
        here = at_rows(c)
        decay = rate - forget[:, here]
        running = jnp.dot(decay, summing, precision=exact, preferred_element_type=F32)
        by_row = lax.dot_general(
            causal.astype(F32), decay, (((1,), (1,)), ((), ())), precision=exact, preferred_element_type=F32)
        last = running[:, rows - 1 :]
        before = offset[...]

        own_copy(c).wait()
        d_arrival(c, 0).wait_recv()
        own_side = pl.ds(pl.multiple_of(chip * 2 * width, 2 * width), 2 * width)
        piece = x[here, own_side]
        for i in range(4):
            partial[i] = jnp.dot(piece, w[i, own_side, :], preferred_element_type=F32)
        if relay:
            @pl.when(jnp.logical_and(place == 1, c == chunks // 4))
            def _():
                hop_copy(0).wait_recv()
                hop_copy(1).start()

        for step in range(1, chips):
            y_arrival(c, step).wait_recv()
            d_copy(c, step).start()
        for step in range(1, chips):
            piece = x[here, columns(back(step))]
            for i in range(4):
                partial[i] += jnp.dot(piece, w[i, columns(back(step)), :], preferred_element_type=F32)
        for step in range(1, chips):
            d_arrival(c, step).wait_recv()

        def project(i):
            total = partial[i]
            for step in range(1, chips):
                total += jnp.dot(
                    x[here, columns(back_other(step))], w[i, columns(back_other(step)), :],
                    preferred_element_type=F32)
            return total

        key = (project(0) * DH ** (-0.5)).astype(BF16)
        value = project(1).astype(BF16)
        for h in range(heads):
            part = slice(h * head_width, (h + 1) * head_width)
            k, v = key[:, part], value[:, part]
            end = last[h : h + 1, :]
            grown = state[h]
            held[h] = grown.astype(BF16)
            faded = (k.astype(F32) * jnp.exp(end - by_row[:, h : h + 1])).astype(BF16)
            state[h] = jnp.exp(end) * grown + contract(faded, v, ((0,), (0,)))

        @pl.when(jnp.logical_and(place == 0, c == chunks - 1))
        def _():
            state_out[...] = state[...].astype(BF16)
            if n_seq > 1:
                for g in range(groups):
                    s_copy(g).start()

        query = project(2).astype(BF16)
        for h in range(heads):
            part = slice(h * head_width, (h + 1) * head_width)
            q, k, v = query[:, part], key[:, part], value[:, part]
            col = by_row[:, h : h + 1]
            mask = jnp.exp(jnp.where(causal, col - running[h : h + 1, :], -1e30))
            scores = (contract(q, k, ((1,), (1,))) * mask).astype(BF16)
            qf = q.astype(F32)
            carried = jnp.dot((qf * jnp.exp(col)).astype(BF16), held[h], preferred_element_type=F32)
            local_out[here, part] = jnp.dot(scores, v, preferred_element_type=F32) + carried
            q_in[here, part] = (qf * jnp.exp(col + before[h : h + 1, 0:1])).astype(BF16)
        offset[...] = before + last
        gate = project(3).astype(BF16).astype(F32)
        gates[here, :] = gate / (1.0 + jnp.exp(-gate))

        @pl.when(place == 0)
        def _():
            for g in range(groups):
                finalize(c, g)

    far_steps = (n_mp - 2) * parts

    def in_order(step):
        o = lax.rem(step, n_mp - 2)
        away = (lax.rem(chip + o // 2 + 1, chips) * 2 + lax.rem(core + o, 2)) * parts + step // (n_mp - 2)
        rest = jnp.maximum(step - far_steps, 0)
        home = (chip * 2 + lax.rem(core + 1 + rest, 2)) * parts + rest // 2
        return jnp.where(step < far_steps, away, home)

    if n_seq > 1:
        @pl.when(place > 0)
        def _():
            for g in range(groups):
                part = slice(g * group_heads, (g + 1) * group_heads)
                s_copy(g).wait_recv()
                enter[part] = state_got[part]
                if n_seq > 2:
                    @pl.when(place < n_seq - 1)
                    def _():
                        for h in range(g * group_heads, (g + 1) * group_heads):
                            total = jnp.exp(offset[h : h + 1, 0:1])
                            state_out[h] = (total * enter[h].astype(F32) + state[h]).astype(BF16)
                        s_copy(g).start()

                detour = relay and g == 0
                if detour:
                    finalize(in_order(0), g, True)
                pl.loop(1 if detour else 0, chunks)(lambda step: finalize(in_order(step), g))

    if relay:
        @pl.when(place == 0)
        def _():
            out_hop(0).wait_recv()
            hop_copy(2).start()

    def m_arrival(source, r, g):
        there = got.at[source, at_rows(r), group_columns(g)]
        return pltpu.make_async_remote_copy(
            src_ref=there, dst_ref=there, send_sem=m_send.at[0, 0], recv_sem=m_recv.at[source, r, g],
            device_id={"mp": partner}, device_id_type=MESH)

    def q_arrival(source, r):
        there = sq_got.at[source, r]
        return pltpu.make_async_remote_copy(
            src_ref=there, dst_ref=there, send_sem=q_send.at[0], recv_sem=q_recv.at[source, r],
            device_id={"mp": partner}, device_id_type=MESH)

    sources = [me, partner] + [lax.rem(chip + t, chips) * 2 + lax.rem(core + s, 2) for t in range(1, chips) for s in (0, 1)]

    for r in range(parts):
        for source in sources[1:]:
            q_arrival(source, r).wait_recv()
        total = sq_got[0, r]
        for source in range(1, n_mp):
            total += sq_got[source, r]
        scale = lax.rsqrt(total * (1.0 / (n_mp * width)) + 1e-06)
        scale = jnp.broadcast_to(scale, (8, rows)).T[:, 0:1]
        span = slice(r * rows, (r + 1) * rows)
        for g in range(groups):
            for i, source in enumerate(sources):
                if i > 0:
                    m_arrival(source, r, g).wait_recv()
                part = pl.ds(pl.multiple_of(source * width + g * group_width, group_width), group_width)
                piece = got[source, span, g * group_width : (g + 1) * group_width].astype(F32)
                out[span, part] = (piece * scale * gain[:, part]).astype(BF16)

    @pl.loop(0, chunks)
    def _(c):
        for step in range(1, chips):
            if relay:
                pl.when(c < chunks - 1)(lambda: y_copy(c, step).wait_send())
            else:
                y_copy(c, step).wait_send()
        for step in range(chips):
            d_copy(c, step).wait_send()

        @pl.when(c // parts != me)
        def _():
            q_copy(c).wait_send()
            for g in range(groups):
                m_copy(c, g).wait_send()

    if n_seq > 1:
        @pl.when(place < n_seq - 1)
        def _():
            for g in range(groups):
                s_copy(g).wait_send()

    if relay:
        @pl.when(place == 0)
        def _():
            y_short().wait_send()
            hop_copy(0).wait_send()
            hop_copy(2).wait_send()

        @pl.when(place == 1)
        def _():
            y_copy(chunks - 1, 1).wait_send()
            hop_copy(1).wait_send()


def in_hbm(a):
    return a if a.size == 1 else pltpu.with_memory_space_constraint(a, pltpu.HBM)


def body(n_mp, n_seq, tokens, w_query, w_key, w_value, w_gate, decay_exponent, forget, norm_gain):
    seq_rows, width = tokens.shape
    features = w_query.shape[0]
    heads = decay_exponent.shape[0]
    own_rows = seq_rows // n_mp
    rows = 256 if own_rows % 256 == 0 else own_rows
    chunks, parts = seq_rows // rows, own_rows // rows
    groups = 2 if heads % 2 == 0 else 1
    hbm = pl.BlockSpec(memory_space=pltpu.HBM)
    dma = pltpu.SemaphoreType.DMA
    chips = n_mp // 2
    return pl.pallas_call(
        functools.partial(kernel, n_mp, n_seq, heads, rows, groups),
        out_shape=pltpu.VMEM((own_rows, features), BF16),
        in_specs=[hbm] * 8,
        out_specs=pl.BlockSpec(memory_space=pltpu.VMEM),
        scratch_shapes=[
            pltpu.VMEM((seq_rows, features), BF16),
            pltpu.VMEM((4, features, width), BF16),
            pltpu.VMEM((1, heads), jnp.int32),
            pltpu.VMEM((heads, seq_rows), F32),
            pltpu.VMEM((1, features), F32),
            pltpu.VMEM((4, rows, width), F32),
            pltpu.VMEM((seq_rows, width), F32),
            pltpu.VMEM((seq_rows, width), BF16),
            pltpu.VMEM((seq_rows, width), F32),
            pltpu.VMEM((seq_rows, width), BF16),
            pltpu.VMEM((n_mp, own_rows, width), BF16),
            pltpu.VMEM((chunks, 1, rows), F32),
            pltpu.VMEM((n_mp, parts, 1, rows), F32),
            pltpu.VMEM((heads, DH, DH), F32),
            pltpu.VMEM((heads, DH, DH), BF16),
            pltpu.VMEM((heads, DH, DH), BF16),
            pltpu.VMEM((heads, DH, DH), BF16),
            pltpu.VMEM((heads, DH, DH), BF16),
            pltpu.VMEM((heads, 128), F32),
            pltpu.VMEM((rows // 2, width), BF16),
            pltpu.VMEM((rows, width // groups), BF16),
            dma((4,)),
            dma((3,)),
            dma((chunks,)),
            dma((chunks, chips)),
            dma((chunks, chips)),
            dma((chunks, chips)),
            dma((chunks, chips)),
            dma((groups,)),
            dma((groups,)),
            dma((chunks, groups)),
            dma((n_mp, parts, groups)),
            dma((chunks,)),
            dma((n_mp, parts)),
            dma((3,)),
            dma((2,)),
        ],
        compiler_params=pltpu.CompilerParams(
            collective_id=0, has_side_effects=True, vmem_limit_bytes=48 * 1024 * 1024
        ),
    )(*(in_hbm(a) for a in (tokens, w_query, w_key, w_value, w_gate, decay_exponent[None, :], forget.T, norm_gain[None, :])))


def solution(mesh):
    placed = (
        P(("dp", "seq"), "mp"),
        P(None, "mp"),
        P(None, "mp"),
        P(None, "mp"),
        P(None, "mp"),
        P("mp"),
        P(("dp", "seq"), "mp"),
        P(),
    )
    return jax.shard_map(
        functools.partial(body, mesh.shape["mp"], mesh.shape["seq"]),
        mesh=mesh,
        in_specs=placed,
        out_specs=P(("dp", "seq", "mp"), None),
        check_vma=False,
    )
```

```python
import functools

import jax
import jax.numpy as jnp
from jax import lax
from jax.experimental import pallas as pl
from jax.experimental.pallas import tpu as pltpu
from jax.sharding import PartitionSpec as P

DH = 128
MESH = pl.DeviceIdType.MESH
F32 = jnp.float32
BF16 = jnp.bfloat16


def contract(a, b, dims):
    return lax.dot_general(a, b, ((dims[0], dims[1]), ((), ())), preferred_element_type=F32)


def kernel(
    n_mp, n_seq, heads, rows, groups,
    tokens, wq, wk, wv, wg, exponent_in, forget_in, gain_in, out,
    x, w, exponent, forget, gain, decays, summed, by_rows, partial, local_out, q_in, gates, moved, got, sq_out, sq_got,
    state, held, enter, state_out, state_got, offset, hop_in, hop_out,
    weight_sem, small_sem, own_sem, y_send, y_recv, d_send, d_recv, s_send, s_recv, m_send, m_recv, q_send, q_recv, hop_send, hop_recv,
):
    me = lax.axis_index("mp")
    place = lax.axis_index("seq")
    chips = n_mp // 2
    chip, core = me // 2, me % 2
    partner = chip * 2 + (1 - core)
    seq_rows, width = tokens.shape
    chunks = seq_rows // rows
    own_rows = seq_rows // n_mp
    parts = own_rows // rows
    head_width = width // heads
    group_heads = heads // groups
    group_width = width // groups
    ahead = partial.shape[0]
    relay = n_seq == 2 and chips == 2
    hop_chunk = 3 if chunks > 4 else chunks - 1
    across = [lax.rem(chip + 1, chips) * 2 + core, lax.rem(chip + 1, chips) * 2 + (1 - core)]

    barrier = pltpu.get_barrier_semaphore()
    for other in range(1, n_mp):
        pl.semaphore_signal(barrier, inc=1, device_id={"mp": lax.rem(me + other, n_mp)}, device_id_type=MESH)

    @pl.when(place > 0)
    def _():
        pl.semaphore_signal(barrier, inc=1, device_id={"seq": place - 1}, device_id_type=MESH)

    @pl.when(place < n_seq - 1)
    def _():
        pl.semaphore_signal(barrier, inc=1, device_id={"seq": place + 1}, device_id_type=MESH)

    if relay:
        for there in across:
            pl.semaphore_signal(barrier, inc=1, device_id={"mp": there, "seq": 1 - place}, device_id_type=MESH)

    weights = [pltpu.make_async_copy(src, w.at[i], weight_sem.at[i]) for i, src in enumerate((wk, wv, wq, wg))]
    small = [
        pltpu.make_async_copy(src, dst, small_sem.at[i])
        for i, (src, dst) in enumerate(((exponent_in, exponent), (forget_in, forget), (gain_in, gain)))
    ]

    def columns(block):
        return pl.ds(pl.multiple_of(block * width, width), width)

    def at_rows(c):
        return pl.ds(pl.multiple_of(c * rows, rows), rows)

    def own_copy(c):
        return pltpu.make_async_copy(tokens.at[at_rows(c), :], x.at[at_rows(c), columns(me)], own_sem.at[c])

    def far(step):
        return lax.rem(chip + step, chips) * 2 + core

    def back(step):
        return lax.rem(chip + chips - step, chips) * 2 + core

    def back_other(step):
        return lax.rem(chip + chips - step, chips) * 2 + (1 - core)

    def y_copy(c, step):
        return pltpu.make_async_remote_copy(
            src_ref=tokens.at[at_rows(c), :], dst_ref=x.at[at_rows(c), columns(me)],
            send_sem=y_send.at[c, step], recv_sem=y_recv.at[c, step],
            device_id={"mp": far(step)}, device_id_type=MESH)

    def y_arrival(c, step):
        return pltpu.make_async_remote_copy(
            src_ref=tokens.at[at_rows(c), :], dst_ref=x.at[at_rows(c), columns(back(step))],
            send_sem=y_send.at[c, step], recv_sem=y_recv.at[c, step],
            device_id={"mp": far(step)}, device_id_type=MESH)

    def d_copy(c, step):
        block = me if step == 0 else back(step)
        source = tokens.at[at_rows(c), :] if step == 0 else x.at[at_rows(c), columns(block)]
        return pltpu.make_async_remote_copy(
            src_ref=source, dst_ref=x.at[at_rows(c), columns(block)],
            send_sem=d_send.at[c, step], recv_sem=d_recv.at[c, step],
            device_id={"mp": partner}, device_id_type=MESH)

    def d_arrival(c, step):
        there = x.at[at_rows(c), columns(partner if step == 0 else back_other(step))]
        return pltpu.make_async_remote_copy(
            src_ref=there, dst_ref=there, send_sem=d_send.at[c, step], recv_sem=d_recv.at[c, step],
            device_id={"mp": partner}, device_id_type=MESH)

    def in_hop():
        return pltpu.make_async_remote_copy(
            src_ref=tokens.at[at_rows(hop_chunk), :], dst_ref=hop_in,
            send_sem=y_send.at[hop_chunk, 1], recv_sem=hop_recv.at[2],
            device_id={"mp": across[0], "seq": 1}, device_id_type=MESH)

    def in_next():
        return pltpu.make_async_remote_copy(
            src_ref=hop_in, dst_ref=x.at[at_rows(hop_chunk), columns(across[0])],
            send_sem=hop_send.at[2], recv_sem=y_recv.at[hop_chunk, 1],
            device_id={"seq": 0}, device_id_type=MESH)

    def out_hop(block, to, i):
        return pltpu.make_async_remote_copy(
            src_ref=moved.at[at_rows(block), pl.ds(0, group_width)], dst_ref=hop_out.at[i],
            send_sem=m_send.at[block, 0], recv_sem=hop_recv.at[i],
            device_id={"mp": to, "seq": 0}, device_id_type=MESH)

    def out_next(i):
        return pltpu.make_async_remote_copy(
            src_ref=hop_out.at[i], dst_ref=got.at[across[i], at_rows(0), pl.ds(0, group_width)],
            send_sem=hop_send.at[i], recv_sem=m_recv.at[across[i], 0, 0],
            device_id={"seq": 1}, device_id_type=MESH)

    for copy in small:
        copy.start()
    own_copy(0).start()
    for copy in weights:
        copy.start()
    pl.loop(1, chunks)(lambda c: own_copy(c).start())

    neighbours = jnp.minimum(place, 1) + jnp.minimum(n_seq - 1 - place, 1)
    pl.semaphore_wait(barrier, n_mp - 1 + neighbours + (2 if relay else 0))

    if relay:
        pl.when(place == 0)(lambda: in_hop().start())

    @pl.loop(0, chunks)
    def _(c):
        for step in range(1, chips):
            if relay:
                pl.when(jnp.logical_or(place > 0, c != hop_chunk))(lambda: y_copy(c, step).start())
            else:
                y_copy(c, step).start()
        d_copy(c, 0).start()

    state[...] = jnp.zeros_like(state)
    offset[...] = jnp.zeros_like(offset)
    enter[...] = jnp.zeros_like(enter)

    later = lax.broadcasted_iota(jnp.int32, (rows, rows), 0)
    earlier = lax.broadcasted_iota(jnp.int32, (rows, rows), 1)
    causal = later >= earlier
    summing = (later <= earlier).astype(F32)
    exact = lax.Precision.HIGHEST
    ones = jnp.ones((8, head_width), BF16)

    for copy in small:
        copy.wait()
    spread = jnp.broadcast_to(exponent[...].astype(F32), (heads, heads))
    diagonal = lax.broadcasted_iota(jnp.int32, (heads, heads), 0) == lax.broadcasted_iota(jnp.int32, (heads, heads), 1)
    column = jnp.sum(jnp.where(diagonal, spread, 0.0), axis=1, keepdims=True)
    rate = jnp.log1p(-jnp.exp2(-column))
    for c in range(chunks):
        decays[c * heads : (c + 1) * heads, :] = rate - forget[:, c * rows : (c + 1) * rows]
    every = jnp.dot(decays[...], summing, precision=exact, preferred_element_type=F32)
    turned = every.T
    for c in range(chunks):
        summed[c] = every[c * heads : (c + 1) * heads, :]
        by_rows[c] = turned[:, c * heads : (c + 1) * heads]

    def near(c):
        own_copy(c).wait()
        d_arrival(c, 0).wait_recv()
        own_side = pl.ds(pl.multiple_of(chip * 2 * width, 2 * width), 2 * width)
        piece = x[at_rows(c), own_side]
        slot = lax.rem(c, ahead)
        for i in range(4):
            partial[slot, i] = jnp.dot(piece, w[i, own_side, :], preferred_element_type=F32)

    for copy in weights:
        copy.wait()
    pl.loop(0, ahead)(near)

    def s_copy(g):
        part = pl.ds(g * group_heads, group_heads)
        return pltpu.make_async_remote_copy(
            src_ref=state_out.at[part], dst_ref=state_got.at[part], send_sem=s_send.at[g], recv_sem=s_recv.at[g],
            device_id={"seq": lax.rem(place + 1, n_seq)}, device_id_type=MESH)

    def group_columns(g):
        return pl.ds(g * group_width, group_width)

    def m_copy(block, g):
        to, r = block // parts, lax.rem(block, parts)
        return pltpu.make_async_remote_copy(
            src_ref=moved.at[at_rows(block), group_columns(g)], dst_ref=got.at[me, at_rows(r), group_columns(g)],
            send_sem=m_send.at[block, g], recv_sem=m_recv.at[me, r, g],
            device_id={"mp": to}, device_id_type=MESH)

    def q_copy(block):
        to, r = block // parts, lax.rem(block, parts)
        return pltpu.make_async_remote_copy(
            src_ref=sq_out.at[block], dst_ref=sq_got.at[me, r],
            send_sem=q_send.at[block], recv_sem=q_recv.at[me, r],
            device_id={"mp": to}, device_id_type=MESH)

    def finalize(block, g):
        here = at_rows(block)
        to, r = block // parts, lax.rem(block, parts)
        square = jnp.zeros((rows, head_width), F32)
        for h in range(g * group_heads, (g + 1) * group_heads):
            part = slice(h * head_width, (h + 1) * head_width)
            whole = local_out[here, part] + jnp.dot(q_in[here, part], enter[h], preferred_element_type=F32)
            kept = whole.astype(BF16).astype(F32)
            moved[here, part] = (gates[here, part] * kept).astype(BF16)
            square += kept * kept
        high = square.astype(BF16)
        low = (square - high.astype(F32)).astype(BF16)
        total = (contract(ones, high, ((1,), (1,))) + contract(ones, low, ((1,), (1,))))[0:1, :]
        if g > 0:
            total = total + sq_out[block]
        sq_out[block] = total

        @pl.when(to != me)
        def _():
            if g == groups - 1:
                q_copy(block).start()
            if relay and g == 0:
                detour = jnp.logical_and(jnp.logical_and(place == 1, r == 0), to // 2 != chip)
                pl.when(detour)(lambda: out_hop(block, to, lax.rem(core + to, 2)).start())
                pl.when(jnp.logical_not(detour))(lambda: m_copy(block, g).start())
            else:
                m_copy(block, g).start()

        @pl.when(to == me)
        def _():
            part = slice(g * group_width, (g + 1) * group_width)
            got[me, at_rows(r), part] = moved[here, part]
            if g == groups - 1:
                sq_got[me, r] = total

    far_steps = (n_mp - 2) * parts

    def away(step):
        o = lax.rem(step, n_mp - 2)
        return (lax.rem(chip + o // 2 + 1, chips) * 2 + lax.rem(core + o, 2)) * parts + step // (n_mp - 2)

    def home(step):
        return (chip * 2 + lax.rem(core + 1 + step, 2)) * parts + step // 2

    def enter_state(g):
        part = slice(g * group_heads, (g + 1) * group_heads)
        s_copy(g).wait_recv()
        enter[part] = state_got[part]

    def ready_far(g, low, high):
        @pl.loop(0, far_steps)
        def _(step):
            block = away(lax.rem(step + 2, far_steps))
            pl.when(jnp.logical_and(block >= low, block < high))(lambda: finalize(block, g))

    @pl.loop(0, chunks)
    def _(c):
        here = at_rows(c)
        slot = lax.rem(c, ahead)
        running, by_row = summed[c], by_rows[c]
        last = running[:, rows - 1 :]
        before = offset[...]

        if relay:
            @pl.when(jnp.logical_and(place == 1, c == 1))
            def _():
                in_hop().wait_recv()
                in_next().start()

            @pl.when(jnp.logical_and(place == 1, c == chunks - 1))
            def _():
                ready_far(0, chunks - 2, chunks - 1)
                for g in range(1, groups):
                    enter_state(g)
                    ready_far(g, 0, chunks - 1)

        for step in range(1, chips):
            y_arrival(c, step).wait_recv()
            d_copy(c, step).start()
        for step in range(1, chips):
            piece = x[here, columns(back(step))]
            for i in range(4):
                partial[slot, i] += jnp.dot(piece, w[i, columns(back(step)), :], preferred_element_type=F32)

        @pl.when(jnp.logical_and(place == 0, c > 0))
        def _():
            for g in range(groups):
                finalize(c - 1, g)

        for step in range(1, chips):
            d_arrival(c, step).wait_recv()

        if relay:
            @pl.when(jnp.logical_and(place == 1, c == chunks - 2))
            def _():
                enter_state(0)
                ready_far(0, 0, chunks - 2)

        def project(i):
            total = partial[slot, i]
            for step in range(1, chips):
                total += jnp.dot(
                    x[here, columns(back_other(step))], w[i, columns(back_other(step)), :],
                    preferred_element_type=F32)
            return total

        key = (project(0) * DH ** (-0.5)).astype(BF16)
        value = project(1).astype(BF16)
        for h in range(heads):
            part = slice(h * head_width, (h + 1) * head_width)
            k, v = key[:, part], value[:, part]
            end = last[h : h + 1, :]
            grown = state[h]
            held[h] = grown.astype(BF16)
            faded = (k.astype(F32) * jnp.exp(end - by_row[:, h : h + 1])).astype(BF16)
            state[h] = jnp.exp(end) * grown + contract(faded, v, ((0,), (0,)))

        @pl.when(jnp.logical_and(place == 0, c == chunks - 1))
        def _():
            state_out[...] = state[...].astype(BF16)
            if n_seq > 1:
                for g in range(groups):
                    s_copy(g).start()

        query = project(2).astype(BF16)
        for h in range(heads):
            part = slice(h * head_width, (h + 1) * head_width)
            q, k, v = query[:, part], key[:, part], value[:, part]
            col = by_row[:, h : h + 1]
            mask = jnp.exp(jnp.where(causal, col - running[h : h + 1, :], -1e30))
            scores = (contract(q, k, ((1,), (1,))) * mask).astype(BF16)
            qf = q.astype(F32)
            carried = jnp.dot((qf * jnp.exp(col)).astype(BF16), held[h], preferred_element_type=F32)
            local_out[here, part] = jnp.dot(scores, v, preferred_element_type=F32) + carried
            q_in[here, part] = (qf * jnp.exp(col + before[h : h + 1, 0:1])).astype(BF16)
        offset[...] = before + last
        gate = project(3).astype(BF16).astype(F32)
        gates[here, :] = gate / (1.0 + jnp.exp(-gate))

        pl.when(c < chunks - ahead)(lambda: near(c + ahead))

    @pl.when(place == 0)
    def _():
        for g in range(groups):
            finalize(chunks - 1, g)

    if n_seq > 1:
        @pl.when(place > 0)
        def _():
            for g in range(groups):
                if relay:
                    pl.when((chunks - 1) // parts // 2 != chip)(lambda: finalize(chunks - 1, g))
                    continue
                enter_state(g)
                if n_seq > 2:
                    @pl.when(place < n_seq - 1)
                    def _():
                        for h in range(g * group_heads, (g + 1) * group_heads):
                            total = jnp.exp(offset[h : h + 1, 0:1])
                            state_out[h] = (total * enter[h].astype(F32) + state[h]).astype(BF16)
                        s_copy(g).start()

                pl.loop(0, far_steps)(lambda step: finalize(away(step), g))

            @pl.loop(0, 2 * parts)
            def _(step):
                for g in range(groups):
                    finalize(home(step), g)

    if relay:
        @pl.when(place == 0)
        def _():
            for i in range(2):
                out_hop(0, across[i], i).wait_recv()
                out_next(i).start()

    def m_arrival(source, r, g):
        there = got.at[source, at_rows(r), group_columns(g)]
        return pltpu.make_async_remote_copy(
            src_ref=there, dst_ref=there, send_sem=m_send.at[0, 0], recv_sem=m_recv.at[source, r, g],
            device_id={"mp": partner}, device_id_type=MESH)

    def q_arrival(source, r):
        there = sq_got.at[source, r]
        return pltpu.make_async_remote_copy(
            src_ref=there, dst_ref=there, send_sem=q_send.at[0], recv_sem=q_recv.at[source, r],
            device_id={"mp": partner}, device_id_type=MESH)

    sources = [me, partner] + [lax.rem(chip + t, chips) * 2 + lax.rem(core + s, 2) for t in range(1, chips) for s in (0, 1)]

    for r in range(parts):
        for source in sources[1:]:
            q_arrival(source, r).wait_recv()
        total = sq_got[0, r]
        for source in range(1, n_mp):
            total += sq_got[source, r]
        scale = lax.rsqrt(total * (1.0 / (n_mp * width)) + 1e-06)
        scale = jnp.broadcast_to(scale, (8, rows)).T[:, 0:1]
        span = slice(r * rows, (r + 1) * rows)
        for g in range(groups):
            for i, source in enumerate(sources):
                if i > 0:
                    m_arrival(source, r, g).wait_recv()
                part = pl.ds(pl.multiple_of(source * width + g * group_width, group_width), group_width)
                piece = got[source, span, g * group_width : (g + 1) * group_width].astype(F32)
                out[span, part] = (piece * scale * gain[:, part]).astype(BF16)

    @pl.loop(0, chunks)
    def _(c):
        for step in range(1, chips):
            y_copy(c, step).wait_send()
        for step in range(chips):
            d_copy(c, step).wait_send()

        @pl.when(c // parts != me)
        def _():
            q_copy(c).wait_send()
            for g in range(groups):
                m_copy(c, g).wait_send()

    if n_seq > 1:
        @pl.when(place < n_seq - 1)
        def _():
            for g in range(groups):
                s_copy(g).wait_send()

    if relay:
        @pl.when(place == 0)
        def _():
            for i in range(2):
                out_next(i).wait_send()

        pl.when(place == 1)(lambda: in_next().wait_send())


def in_hbm(a):
    return a if a.size == 1 else pltpu.with_memory_space_constraint(a, pltpu.HBM)


def body(n_mp, n_seq, tokens, w_query, w_key, w_value, w_gate, decay_exponent, forget, norm_gain):
    seq_rows, width = tokens.shape
    features = w_query.shape[0]
    heads = decay_exponent.shape[0]
    own_rows = seq_rows // n_mp
    rows = 256 if own_rows % 256 == 0 else own_rows
    chunks, parts = seq_rows // rows, own_rows // rows
    groups = 2 if heads % 2 == 0 else 1
    hbm = pl.BlockSpec(memory_space=pltpu.HBM)
    dma = pltpu.SemaphoreType.DMA
    chips = n_mp // 2
    return pl.pallas_call(
        functools.partial(kernel, n_mp, n_seq, heads, rows, groups),
        out_shape=pltpu.VMEM((own_rows, features), BF16),
        in_specs=[hbm] * 8,
        out_specs=pl.BlockSpec(memory_space=pltpu.VMEM),
        scratch_shapes=[
            pltpu.VMEM((seq_rows, features), BF16),
            pltpu.VMEM((4, features, width), BF16),
            pltpu.VMEM((1, heads), jnp.int32),
            pltpu.VMEM((heads, seq_rows), F32),
            pltpu.VMEM((1, features), F32),
            pltpu.VMEM((chunks * heads, rows), F32),
            pltpu.VMEM((chunks, heads, rows), F32),
            pltpu.VMEM((chunks, rows, heads), F32),
            pltpu.VMEM((4, 4, rows, width), F32),
            pltpu.VMEM((seq_rows, width), F32),
            pltpu.VMEM((seq_rows, width), BF16),
            pltpu.VMEM((seq_rows, width), F32),
            pltpu.VMEM((seq_rows, width), BF16),
            pltpu.VMEM((n_mp, own_rows, width), BF16),
            pltpu.VMEM((chunks, 1, rows), F32),
            pltpu.VMEM((n_mp, parts, 1, rows), F32),
            pltpu.VMEM((heads, DH, DH), F32),
            pltpu.VMEM((heads, DH, DH), BF16),
            pltpu.VMEM((heads, DH, DH), BF16),
            pltpu.VMEM((heads, DH, DH), BF16),
            pltpu.VMEM((heads, DH, DH), BF16),
            pltpu.VMEM((heads, 128), F32),
            pltpu.VMEM((rows, width), BF16),
            pltpu.VMEM((2, rows, width // groups), BF16),
            dma((4,)),
            dma((3,)),
            dma((chunks,)),
            dma((chunks, chips)),
            dma((chunks, chips)),
            dma((chunks, chips)),
            dma((chunks, chips)),
            dma((groups,)),
            dma((groups,)),
            dma((chunks, groups)),
            dma((n_mp, parts, groups)),
            dma((chunks,)),
            dma((n_mp, parts)),
            dma((3,)),
            dma((3,)),
        ],
        compiler_params=pltpu.CompilerParams(
            collective_id=0, has_side_effects=True, vmem_limit_bytes=56 * 1024 * 1024
        ),
    )(*(in_hbm(a) for a in (tokens, w_query, w_key, w_value, w_gate, decay_exponent[None, :], forget.T, norm_gain[None, :])))


def solution(mesh):
    placed = (
        P(("dp", "seq"), "mp"),
        P(None, "mp"),
        P(None, "mp"),
        P(None, "mp"),
        P(None, "mp"),
        P("mp"),
        P(("dp", "seq"), "mp"),
        P(),
    )
    return jax.shard_map(
        functools.partial(body, mesh.shape["mp"], mesh.shape["seq"]),
        mesh=mesh,
        in_specs=placed,
        out_specs=P(("dp", "seq", "mp"), None),
        check_vma=False,
    )
```

```python
import functools

import jax
import jax.numpy as jnp
from jax import lax
from jax.experimental import pallas as pl
from jax.experimental.pallas import tpu as pltpu
from jax.sharding import PartitionSpec as P

DH = 128
MESH = pl.DeviceIdType.MESH
F32 = jnp.float32
BF16 = jnp.bfloat16


def contract(a, b, dims):
    return lax.dot_general(a, b, ((dims[0], dims[1]), ((), ())), preferred_element_type=F32)


def kernel(
    n_mp, n_seq, heads, rows, groups,
    tokens, wq, wk, wv, wg, exponent_in, forget_in, gain_in, out,
    x, w, exponent, forget, gain, decays, summed, by_rows, partial, local_out, q_in, gates, moved, got, sq_out, sq_got,
    state, held, enter, state_out, state_got, offset, hop_in, hop_out,
    weight_sem, small_sem, own_sem, y_send, y_recv, p_send, p_recv, d_send, d_recv, s_send, s_recv, m_send, m_recv, q_send, q_recv, hop_send, hop_recv,
):
    me = lax.axis_index("mp")
    place = lax.axis_index("seq")
    chips = n_mp // 2
    chip, core = me // 2, me % 2
    partner = chip * 2 + (1 - core)
    seq_rows, width = tokens.shape
    chunks = seq_rows // rows
    own_rows = seq_rows // n_mp
    parts = own_rows // rows
    head_width = width // heads
    group_heads = heads // groups
    group_width = width // groups
    ahead = partial.shape[0]
    relay = n_seq == 2 and chips == 2
    hop_chunk = 3 if chunks > 4 else chunks - 1
    across = [lax.rem(chip + 1, chips) * 2 + core, lax.rem(chip + 1, chips) * 2 + (1 - core)]

    barrier = pltpu.get_barrier_semaphore()
    for other in range(1, n_mp):
        pl.semaphore_signal(barrier, inc=1, device_id={"mp": lax.rem(me + other, n_mp)}, device_id_type=MESH)

    @pl.when(place > 0)
    def _():
        pl.semaphore_signal(barrier, inc=1, device_id={"seq": place - 1}, device_id_type=MESH)

    @pl.when(place < n_seq - 1)
    def _():
        pl.semaphore_signal(barrier, inc=1, device_id={"seq": place + 1}, device_id_type=MESH)

    if relay:
        for there in across:
            pl.semaphore_signal(barrier, inc=1, device_id={"mp": there, "seq": 1 - place}, device_id_type=MESH)

    weights = [pltpu.make_async_copy(src, w.at[i], weight_sem) for i, src in enumerate((wk, wv, wq, wg))]
    small = [
        pltpu.make_async_copy(src, dst, small_sem.at[i])
        for i, (src, dst) in enumerate(((exponent_in, exponent), (forget_in, forget), (gain_in, gain)))
    ]

    def columns(block):
        return pl.ds(pl.multiple_of(block * width, width), width)

    def at_rows(c):
        return pl.ds(pl.multiple_of(c * rows, rows), rows)

    def own_copy():
        return pltpu.make_async_copy(tokens, x.at[:, columns(me)], own_sem)

    def far(step):
        return lax.rem(chip + step, chips) * 2 + core

    def back(step):
        return lax.rem(chip + chips - step, chips) * 2 + core

    def back_other(step):
        return lax.rem(chip + chips - step, chips) * 2 + (1 - core)

    def y_copy(c, step):
        return pltpu.make_async_remote_copy(
            src_ref=tokens.at[at_rows(c), :], dst_ref=x.at[at_rows(c), columns(me)],
            send_sem=y_send.at[step - 1], recv_sem=y_recv.at[c, step - 1],
            device_id={"mp": far(step)}, device_id_type=MESH)

    def y_arrival(c, step):
        return pltpu.make_async_remote_copy(
            src_ref=tokens.at[at_rows(c), :], dst_ref=x.at[at_rows(c), columns(back(step))],
            send_sem=y_send.at[step - 1], recv_sem=y_recv.at[c, step - 1],
            device_id={"mp": far(step)}, device_id_type=MESH)

    def at_pair(i):
        return pl.ds(pl.multiple_of(i * 2 * rows, 2 * rows), 2 * rows)

    def p_copy(i):
        return pltpu.make_async_remote_copy(
            src_ref=tokens.at[at_pair(i), :], dst_ref=x.at[at_pair(i), columns(me)],
            send_sem=p_send, recv_sem=p_recv.at[i],
            device_id={"mp": partner}, device_id_type=MESH)

    def p_arrival(i):
        there = x.at[at_pair(i), columns(partner)]
        return pltpu.make_async_remote_copy(
            src_ref=there, dst_ref=there, send_sem=p_send, recv_sem=p_recv.at[i],
            device_id={"mp": partner}, device_id_type=MESH)

    def d_copy(c, step):
        there = x.at[at_rows(c), columns(back(step))]
        return pltpu.make_async_remote_copy(
            src_ref=there, dst_ref=there, send_sem=d_send.at[step - 1], recv_sem=d_recv.at[c, step - 1],
            device_id={"mp": partner}, device_id_type=MESH)

    def d_arrival(c, step):
        there = x.at[at_rows(c), columns(back_other(step))]
        return pltpu.make_async_remote_copy(
            src_ref=there, dst_ref=there, send_sem=d_send.at[step - 1], recv_sem=d_recv.at[c, step - 1],
            device_id={"mp": partner}, device_id_type=MESH)

    def in_hop():
        return pltpu.make_async_remote_copy(
            src_ref=tokens.at[at_rows(hop_chunk), :], dst_ref=hop_in,
            send_sem=y_send.at[0], recv_sem=hop_recv.at[0],
            device_id={"mp": across[0], "seq": 1}, device_id_type=MESH)

    def in_next():
        return pltpu.make_async_remote_copy(
            src_ref=hop_in, dst_ref=x.at[at_rows(hop_chunk), columns(across[0])],
            send_sem=hop_send, recv_sem=y_recv.at[hop_chunk, 0],
            device_id={"seq": 0}, device_id_type=MESH)

    def out_hop(block, to, i):
        return pltpu.make_async_remote_copy(
            src_ref=moved.at[at_rows(block), pl.ds(0, group_width)], dst_ref=hop_out.at[i],
            send_sem=m_send, recv_sem=hop_recv.at[i],
            device_id={"mp": to, "seq": 0}, device_id_type=MESH)

    def out_next(i):
        return pltpu.make_async_remote_copy(
            src_ref=hop_out.at[i], dst_ref=got.at[across[i], at_rows(0), pl.ds(0, group_width)],
            send_sem=hop_send, recv_sem=m_recv.at[across[i], 0],
            device_id={"seq": 1}, device_id_type=MESH)

    for copy in small:
        copy.start()
    own_copy().start()
    for copy in weights:
        copy.start()

    neighbours = jnp.minimum(place, 1) + jnp.minimum(n_seq - 1 - place, 1)
    pl.semaphore_wait(barrier, n_mp - 1 + neighbours + (2 if relay else 0))

    if relay:
        pl.when(place == 0)(lambda: in_hop().start())

    @pl.loop(0, chunks)
    def _(c):
        for step in range(1, chips):
            if relay:
                pl.when(jnp.logical_or(place > 0, c != hop_chunk))(lambda: y_copy(c, step).start())
            else:
                y_copy(c, step).start()
        pl.when(lax.rem(c, 2) == 0)(lambda: p_copy(c // 2).start())

    state[...] = jnp.zeros_like(state)
    offset[...] = jnp.zeros_like(offset)
    enter[...] = jnp.zeros_like(enter)

    later = lax.broadcasted_iota(jnp.int32, (rows, rows), 0)
    earlier = lax.broadcasted_iota(jnp.int32, (rows, rows), 1)
    causal = later >= earlier
    summing = (later <= earlier).astype(F32)
    exact = lax.Precision.HIGHEST
    ones = jnp.ones((8, head_width), BF16)

    for copy in small:
        copy.wait()
    spread = jnp.broadcast_to(exponent[...].astype(F32), (heads, heads))
    diagonal = lax.broadcasted_iota(jnp.int32, (heads, heads), 0) == lax.broadcasted_iota(jnp.int32, (heads, heads), 1)
    column = jnp.sum(jnp.where(diagonal, spread, 0.0), axis=1, keepdims=True)
    rate = jnp.log1p(-jnp.exp2(-column))
    for c in range(chunks):
        decays[c * heads : (c + 1) * heads, :] = rate - forget[:, c * rows : (c + 1) * rows]
    every = jnp.dot(decays[...], summing, precision=exact, preferred_element_type=F32)
    turned = every.T
    for c in range(chunks):
        summed[c] = every[c * heads : (c + 1) * heads, :]
        by_rows[c] = turned[:, c * heads : (c + 1) * heads]

    def near(c):
        pl.when(lax.rem(c, 2) == 0)(lambda: p_arrival(c // 2).wait_recv())
        own_side = pl.ds(pl.multiple_of(chip * 2 * width, 2 * width), 2 * width)
        piece = x[at_rows(c), own_side]
        slot = lax.rem(c, ahead)
        for i in range(4):
            partial[slot, i] = jnp.dot(piece, w[i, own_side, :], preferred_element_type=F32)

    own_copy().wait()
    pltpu.make_async_copy(w, w, weight_sem).wait()
    pl.loop(0, ahead)(near)

    def s_copy(g):
        part = pl.ds(g * group_heads, group_heads)
        return pltpu.make_async_remote_copy(
            src_ref=state_out.at[part], dst_ref=state_got.at[part], send_sem=s_send, recv_sem=s_recv.at[g],
            device_id={"seq": lax.rem(place + 1, n_seq)}, device_id_type=MESH)

    def group_columns(g):
        return pl.ds(g * group_width, group_width)

    def m_copy(block, g):
        to, r = block // parts, lax.rem(block, parts)
        return pltpu.make_async_remote_copy(
            src_ref=moved.at[at_rows(block), group_columns(g)], dst_ref=got.at[me, at_rows(r), group_columns(g)],
            send_sem=m_send, recv_sem=m_recv.at[me, r],
            device_id={"mp": to}, device_id_type=MESH)

    def q_copy(block):
        to, r = block // parts, lax.rem(block, parts)
        return pltpu.make_async_remote_copy(
            src_ref=sq_out.at[block], dst_ref=sq_got.at[r, me],
            send_sem=q_send, recv_sem=q_recv.at[r],
            device_id={"mp": to}, device_id_type=MESH)

    def finalize(block, g):
        here = at_rows(block)
        to, r = block // parts, lax.rem(block, parts)
        square = jnp.zeros((rows, head_width), F32)
        for h in range(g * group_heads, (g + 1) * group_heads):
            part = slice(h * head_width, (h + 1) * head_width)
            whole = local_out[here, part] + jnp.dot(q_in[here, part], enter[h], preferred_element_type=F32)
            kept = whole.astype(BF16).astype(F32)
            moved[here, part] = (gates[here, part] * kept).astype(BF16)
            square += kept * kept
        high = square.astype(BF16)
        low = (square - high.astype(F32)).astype(BF16)
        total = (contract(ones, high, ((1,), (1,))) + contract(ones, low, ((1,), (1,))))[0:1, :]
        if g > 0:
            total = total + sq_out[block]
        sq_out[block] = total

        @pl.when(to != me)
        def _():
            if g == groups - 1:
                q_copy(block).start()
            if relay and g == 0:
                detour = jnp.logical_and(jnp.logical_and(place == 1, r == 0), to // 2 != chip)
                pl.when(detour)(lambda: out_hop(block, to, lax.rem(core + to, 2)).start())
                pl.when(jnp.logical_not(detour))(lambda: m_copy(block, g).start())
            else:
                m_copy(block, g).start()

        @pl.when(to == me)
        def _():
            part = slice(g * group_width, (g + 1) * group_width)
            got[me, at_rows(r), part] = moved[here, part]
            if g == groups - 1:
                sq_got[r, me] = total

    far_steps = (n_mp - 2) * parts

    def away(step):
        o = lax.rem(step, n_mp - 2)
        return (lax.rem(chip + o // 2 + 1, chips) * 2 + lax.rem(core + o, 2)) * parts + step // (n_mp - 2)

    def home(step):
        return (chip * 2 + lax.rem(core + 1 + step, 2)) * parts + step // 2

    def enter_state(g):
        part = slice(g * group_heads, (g + 1) * group_heads)
        s_copy(g).wait_recv()
        enter[part] = state_got[part]

    def ready_far(g, low, high):
        @pl.loop(0, far_steps)
        def _(step):
            block = away(lax.rem(step + 2, far_steps))
            pl.when(jnp.logical_and(block >= low, block < high))(lambda: finalize(block, g))

    @pl.loop(0, chunks)
    def _(c):
        here = at_rows(c)
        slot = lax.rem(c, ahead)
        running, by_row = summed[c], by_rows[c]
        last = running[:, rows - 1 :]
        before = offset[...]

        if relay:
            @pl.when(jnp.logical_and(place == 1, c == 1))
            def _():
                in_hop().wait_recv()
                in_next().start()

            @pl.when(jnp.logical_and(place == 1, c == chunks - 1))
            def _():
                ready_far(0, chunks - 2, chunks - 1)
                for g in range(1, groups):
                    enter_state(g)
                    ready_far(g, 0, chunks - 1)

        for step in range(1, chips):
            y_arrival(c, step).wait_recv()
            d_copy(c, step).start()
        for step in range(1, chips):
            piece = x[here, columns(back(step))]
            for i in range(4):
                partial[slot, i] += jnp.dot(piece, w[i, columns(back(step)), :], preferred_element_type=F32)

        @pl.when(jnp.logical_and(place == 0, c > 0))
        def _():
            for g in range(groups):
                finalize(c - 1, g)

        for step in range(1, chips):
            d_arrival(c, step).wait_recv()

        if relay:
            @pl.when(jnp.logical_and(place == 1, c == chunks - 2))
            def _():
                enter_state(0)
                ready_far(0, 0, chunks - 2)

        def project(i):
            total = partial[slot, i]
            for step in range(1, chips):
                total += jnp.dot(
                    x[here, columns(back_other(step))], w[i, columns(back_other(step)), :],
                    preferred_element_type=F32)
            return total

        key = (project(0) * DH ** (-0.5)).astype(BF16)
        value = project(1).astype(BF16)
        for h in range(heads):
            part = slice(h * head_width, (h + 1) * head_width)
            k, v = key[:, part], value[:, part]
            end = last[h : h + 1, :]
            grown = state[h]
            held[h] = grown.astype(BF16)
            faded = (k.astype(F32) * jnp.exp(end - by_row[:, h : h + 1])).astype(BF16)
            state[h] = jnp.exp(end) * grown + contract(faded, v, ((0,), (0,)))

        @pl.when(jnp.logical_and(place == 0, c == chunks - 1))
        def _():
            state_out[...] = state[...].astype(BF16)
            if n_seq > 1:
                for g in range(groups):
                    s_copy(g).start()

        query = project(2).astype(BF16)
        for h in range(heads):
            part = slice(h * head_width, (h + 1) * head_width)
            q, k, v = query[:, part], key[:, part], value[:, part]
            col = by_row[:, h : h + 1]
            mask = jnp.exp(jnp.where(causal, col - running[h : h + 1, :], -1e30))
            scores = (contract(q, k, ((1,), (1,))) * mask).astype(BF16)
            qf = q.astype(F32)
            carried = jnp.dot((qf * jnp.exp(col)).astype(BF16), held[h], preferred_element_type=F32)
            local_out[here, part] = jnp.dot(scores, v, preferred_element_type=F32) + carried
            q_in[here, part] = (qf * jnp.exp(col + before[h : h + 1, 0:1])).astype(BF16)
        offset[...] = before + last
        gate = project(3).astype(BF16).astype(F32)
        gates[here, :] = gate / (1.0 + jnp.exp(-gate))

        pl.when(c < chunks - ahead)(lambda: near(c + ahead))

    @pl.when(place == 0)
    def _():
        for g in range(groups):
            finalize(chunks - 1, g)

    if n_seq > 1:
        @pl.when(place > 0)
        def _():
            for g in range(groups):
                if relay:
                    pl.when((chunks - 1) // parts // 2 != chip)(lambda: finalize(chunks - 1, g))
                    continue
                enter_state(g)
                if n_seq > 2:
                    @pl.when(place < n_seq - 1)
                    def _():
                        for h in range(g * group_heads, (g + 1) * group_heads):
                            total = jnp.exp(offset[h : h + 1, 0:1])
                            state_out[h] = (total * enter[h].astype(F32) + state[h]).astype(BF16)
                        s_copy(g).start()

                pl.loop(0, far_steps)(lambda step: finalize(away(step), g))

            @pl.loop(0, 2 * parts)
            def _(step):
                for g in range(groups):
                    finalize(home(step), g)

    if relay:
        @pl.when(place == 0)
        def _():
            for i in range(2):
                out_hop(0, across[i], i).wait_recv()
                out_next(i).start()

    def m_arrival(source, r):
        there = got.at[source, at_rows(r), :]
        return pltpu.make_async_remote_copy(
            src_ref=there, dst_ref=there, send_sem=m_send, recv_sem=m_recv.at[source, r],
            device_id={"mp": partner}, device_id_type=MESH)

    def q_arrival(r):
        there = sq_got.at[r, pl.ds(0, n_mp - 1)]
        return pltpu.make_async_remote_copy(
            src_ref=there, dst_ref=there, send_sem=q_send, recv_sem=q_recv.at[r],
            device_id={"mp": partner}, device_id_type=MESH)

    sources = [me, partner] + [lax.rem(chip + t, chips) * 2 + lax.rem(core + s, 2) for t in range(1, chips) for s in (0, 1)]

    for r in range(parts):
        q_arrival(r).wait_recv()
        total = sq_got[r, 0]
        for source in range(1, n_mp):
            total += sq_got[r, source]
        scale = lax.rsqrt(total * (1.0 / (n_mp * width)) + 1e-06)
        scale = jnp.broadcast_to(scale, (8, rows)).T[:, 0:1]
        span = slice(r * rows, (r + 1) * rows)
        for i, source in enumerate(sources):
            if i > 0:
                m_arrival(source, r).wait_recv()
            out[span, columns(source)] = (got[source, span, :].astype(F32) * scale * gain[:, columns(source)]).astype(BF16)

    def sent(ref, sem):
        pltpu.make_async_remote_copy(
            src_ref=ref, dst_ref=ref, send_sem=sem, recv_sem=own_sem,
            device_id={"mp": partner}, device_id_type=MESH).wait_send()

    for step in range(1, chips):
        sent(tokens, y_send.at[step - 1])
        sent(x.at[:, columns(0)], d_send.at[step - 1])
    sent(tokens, p_send)
    sent(sq_out.at[pl.ds(0, chunks - parts)], q_send)
    sent(moved.at[pl.ds(0, seq_rows - own_rows), :], m_send)
    if n_seq > 1:
        pl.when(place < n_seq - 1)(lambda: sent(state_out, s_send))
    if relay:
        pl.when(place == 0)(lambda: sent(hop_out, hop_send))
        pl.when(place == 1)(lambda: sent(hop_in, hop_send))


def in_hbm(a):
    return a if a.size == 1 else pltpu.with_memory_space_constraint(a, pltpu.HBM)


def body(n_mp, n_seq, tokens, w_query, w_key, w_value, w_gate, decay_exponent, forget, norm_gain):
    seq_rows, width = tokens.shape
    features = w_query.shape[0]
    heads = decay_exponent.shape[0]
    own_rows = seq_rows // n_mp
    rows = 256 if own_rows % 256 == 0 else own_rows
    chunks, parts = seq_rows // rows, own_rows // rows
    groups = 2 if heads % 2 == 0 else 1
    hbm = pl.BlockSpec(memory_space=pltpu.HBM)
    dma = pltpu.SemaphoreType.DMA
    chips = n_mp // 2
    return pl.pallas_call(
        functools.partial(kernel, n_mp, n_seq, heads, rows, groups),
        out_shape=pltpu.VMEM((own_rows, features), BF16),
        in_specs=[hbm] * 8,
        out_specs=pl.BlockSpec(memory_space=pltpu.VMEM),
        scratch_shapes=[
            pltpu.VMEM((seq_rows, features), BF16),
            pltpu.VMEM((4, features, width), BF16),
            pltpu.VMEM((1, heads), jnp.int32),
            pltpu.VMEM((heads, seq_rows), F32),
            pltpu.VMEM((1, features), F32),
            pltpu.VMEM((chunks * heads, rows), F32),
            pltpu.VMEM((chunks, heads, rows), F32),
            pltpu.VMEM((chunks, rows, heads), F32),
            pltpu.VMEM((4, 4, rows, width), F32),
            pltpu.VMEM((seq_rows, width), F32),
            pltpu.VMEM((seq_rows, width), BF16),
            pltpu.VMEM((seq_rows, width), F32),
            pltpu.VMEM((seq_rows, width), BF16),
            pltpu.VMEM((n_mp, own_rows, width), BF16),
            pltpu.VMEM((chunks, 1, rows), F32),
            pltpu.VMEM((parts, n_mp, 1, rows), F32),
            pltpu.VMEM((heads, DH, DH), F32),
            pltpu.VMEM((heads, DH, DH), BF16),
            pltpu.VMEM((heads, DH, DH), BF16),
            pltpu.VMEM((heads, DH, DH), BF16),
            pltpu.VMEM((heads, DH, DH), BF16),
            pltpu.VMEM((heads, 128), F32),
            pltpu.VMEM((rows, width), BF16),
            pltpu.VMEM((2, rows, width // groups), BF16),
            dma,
            dma((3,)),
            dma,
            dma((chips - 1,)),
            dma((chunks, chips - 1)),
            dma,
            dma((chunks // 2,)),
            dma((chips - 1,)),
            dma((chunks, chips - 1)),
            dma,
            dma((groups,)),
            dma,
            dma((n_mp, parts)),
            dma,
            dma((parts,)),
            dma,
            dma((2,)),
        ],
        compiler_params=pltpu.CompilerParams(
            collective_id=0, has_side_effects=True, vmem_limit_bytes=56 * 1024 * 1024
        ),
    )(*(in_hbm(a) for a in (tokens, w_query, w_key, w_value, w_gate, decay_exponent[None, :], forget.T, norm_gain[None, :])))


def solution(mesh):
    placed = (
        P(("dp", "seq"), "mp"),
        P(None, "mp"),
        P(None, "mp"),
        P(None, "mp"),
        P(None, "mp"),
        P("mp"),
        P(("dp", "seq"), "mp"),
        P(),
    )
    return jax.shard_map(
        functools.partial(body, mesh.shape["mp"], mesh.shape["seq"]),
        mesh=mesh,
        in_specs=placed,
        out_specs=P(("dp", "seq", "mp"), None),
        check_vma=False,
    )
```

```python
import functools

import jax
import jax.numpy as jnp
from jax import lax
from jax.experimental import pallas as pl
from jax.experimental.pallas import tpu as pltpu
from jax.sharding import PartitionSpec as P

DH = 128
MESH = pl.DeviceIdType.MESH
F32 = jnp.float32
BF16 = jnp.bfloat16


def contract(a, b, dims):
    return lax.dot_general(a, b, ((dims[0], dims[1]), ((), ())), preferred_element_type=F32)


def kernel(
    n_mp, n_seq, heads, rows, groups,
    tokens, wq, wk, wv, wg, exponent_in, forget_in, gain_in, out,
    x, w, exponent, forget, gain, decays, summed, by_rows, partial, local_out, q_in, gates, moved, got, sq_out, sq_got,
    state, held, enter, state_out, state_got, offset, hop_in, hop_out,
    weight_sem, small_sem, own_sem, y_send, y_recv, p_send, p_recv, d_send, d_recv, s_send, s_recv, m_send, m_recv, q_send, q_recv, hop_send, hop_recv, ready,
):
    me = lax.axis_index("mp")
    place = lax.axis_index("seq")
    chips = n_mp // 2
    chip, core = me // 2, me % 2
    partner = chip * 2 + (1 - core)
    seq_rows, width = tokens.shape
    chunks = seq_rows // rows
    own_rows = seq_rows // n_mp
    parts = own_rows // rows
    head_width = width // heads
    group_heads = heads // groups
    group_width = width // groups
    ahead = partial.shape[0]
    relay = n_seq == 2 and chips == 2
    hop_chunk = 3 if chunks > 4 else chunks - 1
    across = [lax.rem(chip + 1, chips) * 2 + core, lax.rem(chip + 1, chips) * 2 + (1 - core)]

    barrier = pltpu.get_barrier_semaphore()
    for other in range(1, n_mp):
        pl.semaphore_signal(barrier, inc=1, device_id={"mp": lax.rem(me + other, n_mp)}, device_id_type=MESH)

    across_place = [{"seq": 1 - place}] + [{"mp": there, "seq": 1 - place} for there in across]

    if relay:
        @pl.when(place == 0)
        def _():
            for there in across_place:
                pl.semaphore_signal(barrier, inc=1, device_id=there, device_id_type=MESH)
    else:
        @pl.when(place > 0)
        def _():
            pl.semaphore_signal(barrier, inc=1, device_id={"seq": place - 1}, device_id_type=MESH)

        @pl.when(place < n_seq - 1)
        def _():
            pl.semaphore_signal(barrier, inc=1, device_id={"seq": place + 1}, device_id_type=MESH)

    weights = [pltpu.make_async_copy(src, w.at[i], weight_sem) for i, src in enumerate((wk, wv, wq, wg))]
    small = [
        pltpu.make_async_copy(src, dst, small_sem.at[i])
        for i, (src, dst) in enumerate(((exponent_in, exponent), (forget_in, forget), (gain_in, gain)))
    ]

    def columns(block):
        return pl.ds(pl.multiple_of(block * width, width), width)

    def at_rows(c):
        return pl.ds(pl.multiple_of(c * rows, rows), rows)

    def own_copy():
        return pltpu.make_async_copy(tokens, x.at[:, columns(me)], own_sem)

    def far(step):
        return lax.rem(chip + step, chips) * 2 + core

    def back(step):
        return lax.rem(chip + chips - step, chips) * 2 + core

    def back_other(step):
        return lax.rem(chip + chips - step, chips) * 2 + (1 - core)

    def y_copy(c, step):
        return pltpu.make_async_remote_copy(
            src_ref=tokens.at[at_rows(c), :], dst_ref=x.at[at_rows(c), columns(me)],
            send_sem=y_send.at[step - 1], recv_sem=y_recv.at[c, step - 1],
            device_id={"mp": far(step)}, device_id_type=MESH)

    def y_arrival(c, step):
        return pltpu.make_async_remote_copy(
            src_ref=tokens.at[at_rows(c), :], dst_ref=x.at[at_rows(c), columns(back(step))],
            send_sem=y_send.at[step - 1], recv_sem=y_recv.at[c, step - 1],
            device_id={"mp": far(step)}, device_id_type=MESH)

    def at_pair(i):
        return pl.ds(pl.multiple_of(i * 2 * rows, 2 * rows), 2 * rows)

    def p_copy(i):
        return pltpu.make_async_remote_copy(
            src_ref=tokens.at[at_pair(i), :], dst_ref=x.at[at_pair(i), columns(me)],
            send_sem=p_send, recv_sem=p_recv.at[i],
            device_id={"mp": partner}, device_id_type=MESH)

    def p_arrival(i):
        there = x.at[at_pair(i), columns(partner)]
        return pltpu.make_async_remote_copy(
            src_ref=there, dst_ref=there, send_sem=p_send, recv_sem=p_recv.at[i],
            device_id={"mp": partner}, device_id_type=MESH)

    def d_copy(c, step):
        there = x.at[at_rows(c), columns(back(step))]
        return pltpu.make_async_remote_copy(
            src_ref=there, dst_ref=there, send_sem=d_send.at[step - 1], recv_sem=d_recv.at[c, step - 1],
            device_id={"mp": partner}, device_id_type=MESH)

    def d_arrival(c, step):
        there = x.at[at_rows(c), columns(back_other(step))]
        return pltpu.make_async_remote_copy(
            src_ref=there, dst_ref=there, send_sem=d_send.at[step - 1], recv_sem=d_recv.at[c, step - 1],
            device_id={"mp": partner}, device_id_type=MESH)

    def in_hop():
        return pltpu.make_async_remote_copy(
            src_ref=tokens.at[at_rows(hop_chunk), :], dst_ref=hop_in,
            send_sem=y_send.at[0], recv_sem=hop_recv.at[0],
            device_id={"mp": across[0], "seq": 1}, device_id_type=MESH)

    def in_next():
        return pltpu.make_async_remote_copy(
            src_ref=hop_in, dst_ref=x.at[at_rows(hop_chunk), columns(across[0])],
            send_sem=hop_send, recv_sem=y_recv.at[hop_chunk, 0],
            device_id={"seq": 0}, device_id_type=MESH)

    hop_rows = hop_out.shape[1]

    def out_hop(block, to, i):
        return pltpu.make_async_remote_copy(
            src_ref=moved.at[pl.ds(pl.multiple_of(block * rows, rows), hop_rows), pl.ds(0, group_width)],
            dst_ref=hop_out.at[i], send_sem=m_send, recv_sem=hop_recv.at[i],
            device_id={"mp": to, "seq": 0}, device_id_type=MESH)

    def out_rest(block, to):
        left = rows - hop_rows
        return pltpu.make_async_remote_copy(
            src_ref=moved.at[pl.ds(pl.multiple_of(block * rows + hop_rows, left), left), pl.ds(0, group_width)],
            dst_ref=got.at[me, pl.ds(hop_rows, left), pl.ds(0, group_width)],
            send_sem=m_send, recv_sem=m_recv.at[me, 0], device_id={"mp": to}, device_id_type=MESH)

    def out_next(i):
        return pltpu.make_async_remote_copy(
            src_ref=hop_out.at[i], dst_ref=got.at[across[i], pl.ds(0, hop_rows), pl.ds(0, group_width)],
            send_sem=hop_send, recv_sem=m_recv.at[across[i], 0],
            device_id={"seq": 1}, device_id_type=MESH)

    for copy in small:
        copy.start()
    own_copy().start()
    for copy in weights:
        copy.start()

    if relay:
        neighbours = place * len(across_place)
    else:
        neighbours = jnp.minimum(place, 1) + jnp.minimum(n_seq - 1 - place, 1)
    pl.semaphore_wait(barrier, n_mp - 1 + neighbours)

    @pl.loop(0, chunks)
    def _(c):
        for step in range(1, chips):
            if relay:
                pl.when(jnp.logical_or(place > 0, c != hop_chunk))(lambda: y_copy(c, step).start())
            else:
                y_copy(c, step).start()
        pl.when(lax.rem(c, 2) == 0)(lambda: p_copy(c // 2).start())

    if relay:
        @pl.when(place == 1)
        def _():
            for there in across_place:
                pl.semaphore_signal(ready, inc=1, device_id=there, device_id_type=MESH)

    state[...] = jnp.zeros_like(state)
    offset[...] = jnp.zeros_like(offset)
    enter[...] = jnp.zeros_like(enter)

    later = lax.broadcasted_iota(jnp.int32, (rows, rows), 0)
    earlier = lax.broadcasted_iota(jnp.int32, (rows, rows), 1)
    causal = later >= earlier
    summing = (later <= earlier).astype(F32)
    exact = lax.Precision.HIGHEST
    ones = jnp.ones((8, head_width), BF16)

    for copy in small:
        copy.wait()
    spread = jnp.broadcast_to(exponent[...].astype(F32), (heads, heads))
    diagonal = lax.broadcasted_iota(jnp.int32, (heads, heads), 0) == lax.broadcasted_iota(jnp.int32, (heads, heads), 1)
    column = jnp.sum(jnp.where(diagonal, spread, 0.0), axis=1, keepdims=True)
    rate = jnp.log1p(-jnp.exp2(-column))
    for c in range(chunks):
        decays[c * heads : (c + 1) * heads, :] = rate - forget[:, c * rows : (c + 1) * rows]
    every = jnp.dot(decays[...], summing, precision=exact, preferred_element_type=F32)
    turned = every.T
    for c in range(chunks):
        summed[c] = every[c * heads : (c + 1) * heads, :]
        by_rows[c] = turned[:, c * heads : (c + 1) * heads]

    def near(c):
        pl.when(lax.rem(c, 2) == 0)(lambda: p_arrival(c // 2).wait_recv())
        own_side = pl.ds(pl.multiple_of(chip * 2 * width, 2 * width), 2 * width)
        piece = x[at_rows(c), own_side]
        slot = lax.rem(c, ahead)
        for i in range(4):
            partial[slot, i] = jnp.dot(piece, w[i, own_side, :], preferred_element_type=F32)

    if relay:
        @pl.when(place == 0)
        def _():
            pl.semaphore_wait(ready, len(across_place))
            in_hop().start()

    own_copy().wait()
    pltpu.make_async_copy(w, w, weight_sem).wait()
    pl.loop(0, ahead)(near)

    def s_copy(g):
        part = pl.ds(g * group_heads, group_heads)
        return pltpu.make_async_remote_copy(
            src_ref=state_out.at[part], dst_ref=state_got.at[part], send_sem=s_send, recv_sem=s_recv.at[g],
            device_id={"seq": lax.rem(place + 1, n_seq)}, device_id_type=MESH)

    def group_columns(g):
        return pl.ds(g * group_width, group_width)

    def m_copy(block, g):
        to, r = block // parts, lax.rem(block, parts)
        return pltpu.make_async_remote_copy(
            src_ref=moved.at[at_rows(block), group_columns(g)], dst_ref=got.at[me, at_rows(r), group_columns(g)],
            send_sem=m_send, recv_sem=m_recv.at[me, r],
            device_id={"mp": to}, device_id_type=MESH)

    def q_copy(block):
        to, r = block // parts, lax.rem(block, parts)
        return pltpu.make_async_remote_copy(
            src_ref=sq_out.at[block], dst_ref=sq_got.at[r, me],
            send_sem=q_send, recv_sem=q_recv.at[r],
            device_id={"mp": to}, device_id_type=MESH)

    def finalize(block, g):
        here = at_rows(block)
        to, r = block // parts, lax.rem(block, parts)
        square = jnp.zeros((rows, head_width), F32)
        for h in range(g * group_heads, (g + 1) * group_heads):
            part = slice(h * head_width, (h + 1) * head_width)
            whole = local_out[here, part] + jnp.dot(q_in[here, part], enter[h], preferred_element_type=F32)
            kept = whole.astype(BF16).astype(F32)
            moved[here, part] = (gates[here, part] * kept).astype(BF16)
            square += kept * kept
        high = square.astype(BF16)
        low = (square - high.astype(F32)).astype(BF16)
        total = (contract(ones, high, ((1,), (1,))) + contract(ones, low, ((1,), (1,))))[0:1, :]
        if g > 0:
            total = total + sq_out[block]
        sq_out[block] = total

        @pl.when(to != me)
        def _():
            if g == groups - 1:
                q_copy(block).start()
            if relay and g == 0:
                detour = jnp.logical_and(jnp.logical_and(place == 1, r == 0), to // 2 != chip)

                @pl.when(detour)
                def _():
                    out_hop(block, to, lax.rem(core + to, 2)).start()
                    out_rest(block, to).start()

                pl.when(jnp.logical_not(detour))(lambda: m_copy(block, g).start())
            else:
                m_copy(block, g).start()

        @pl.when(to == me)
        def _():
            part = slice(g * group_width, (g + 1) * group_width)
            got[me, at_rows(r), part] = moved[here, part]
            if g == groups - 1:
                sq_got[r, me] = total

    far_steps = (n_mp - 2) * parts

    def away(step):
        o = lax.rem(step, n_mp - 2)
        return (lax.rem(chip + o // 2 + 1, chips) * 2 + lax.rem(core + o, 2)) * parts + step // (n_mp - 2)

    def home(step):
        return (chip * 2 + lax.rem(core + 1 + step, 2)) * parts + step // 2

    def enter_state(g):
        part = slice(g * group_heads, (g + 1) * group_heads)
        s_copy(g).wait_recv()
        enter[part] = state_got[part]

    def ready_far(g, low, high):
        @pl.loop(0, far_steps)
        def _(step):
            block = away(lax.rem(step + 2, far_steps) if g == 0 else step)
            pl.when(jnp.logical_and(block >= low, block < high))(lambda: finalize(block, g))

    @pl.loop(0, chunks)
    def _(c):
        here = at_rows(c)
        slot = lax.rem(c, ahead)
        running, by_row = summed[c], by_rows[c]
        last = running[:, rows - 1 :]
        before = offset[...]

        if relay:
            @pl.when(jnp.logical_and(place == 1, c == 1))
            def _():
                in_hop().wait_recv()
                in_next().start()

            @pl.when(jnp.logical_and(place == 1, c == chunks - 1))
            def _():
                ready_far(0, chunks - 2, chunks - 1)
                for g in range(1, groups):
                    enter_state(g)
                    ready_far(g, 0, chunks - 1)

        for step in range(1, chips):
            y_arrival(c, step).wait_recv()
            d_copy(c, step).start()
        for step in range(1, chips):
            piece = x[here, columns(back(step))]
            for i in range(4):
                partial[slot, i] += jnp.dot(piece, w[i, columns(back(step)), :], preferred_element_type=F32)

        @pl.when(jnp.logical_and(place == 0, c > 0))
        def _():
            for g in range(groups):
                finalize(c - 1, g)

        for step in range(1, chips):
            d_arrival(c, step).wait_recv()

        if relay:
            @pl.when(jnp.logical_and(place == 1, c == chunks - 2))
            def _():
                enter_state(0)
                ready_far(0, 0, chunks - 2)

        def project(i):
            total = partial[slot, i]
            for step in range(1, chips):
                total += jnp.dot(
                    x[here, columns(back_other(step))], w[i, columns(back_other(step)), :],
                    preferred_element_type=F32)
            return total

        key = (project(0) * DH ** (-0.5)).astype(BF16)
        value = project(1).astype(BF16)
        for h in range(heads):
            part = slice(h * head_width, (h + 1) * head_width)
            k, v = key[:, part], value[:, part]
            end = last[h : h + 1, :]
            grown = state[h]
            held[h] = grown.astype(BF16)
            faded = (k.astype(F32) * jnp.exp(end - by_row[:, h : h + 1])).astype(BF16)
            state[h] = jnp.exp(end) * grown + contract(faded, v, ((0,), (0,)))

        @pl.when(jnp.logical_and(place == 0, c == chunks - 1))
        def _():
            state_out[...] = state[...].astype(BF16)
            if n_seq > 1:
                for g in range(groups):
                    s_copy(g).start()

        query = project(2).astype(BF16)
        for h in range(heads):
            part = slice(h * head_width, (h + 1) * head_width)
            q, k, v = query[:, part], key[:, part], value[:, part]
            col = by_row[:, h : h + 1]
            mask = jnp.exp(jnp.where(causal, col - running[h : h + 1, :], -1e30))
            scores = (contract(q, k, ((1,), (1,))) * mask).astype(BF16)
            qf = q.astype(F32)
            carried = jnp.dot((qf * jnp.exp(col)).astype(BF16), held[h], preferred_element_type=F32)
            local_out[here, part] = jnp.dot(scores, v, preferred_element_type=F32) + carried
            q_in[here, part] = (qf * jnp.exp(col + before[h : h + 1, 0:1])).astype(BF16)
        offset[...] = before + last
        gate = project(3).astype(BF16).astype(F32)
        gates[here, :] = gate / (1.0 + jnp.exp(-gate))

        pl.when(c < chunks - ahead)(lambda: near(c + ahead))

    @pl.when(place == 0)
    def _():
        for g in range(groups):
            finalize(chunks - 1, g)

    if n_seq > 1:
        @pl.when(place > 0)
        def _():
            for g in range(groups):
                if relay:
                    pl.when((chunks - 1) // parts // 2 != chip)(lambda: finalize(chunks - 1, g))
                    continue
                enter_state(g)
                if n_seq > 2:
                    @pl.when(place < n_seq - 1)
                    def _():
                        for h in range(g * group_heads, (g + 1) * group_heads):
                            total = jnp.exp(offset[h : h + 1, 0:1])
                            state_out[h] = (total * enter[h].astype(F32) + state[h]).astype(BF16)
                        s_copy(g).start()

                pl.loop(0, far_steps)(lambda step: finalize(away(step), g))

            @pl.loop(0, 2 * parts)
            def _(step):
                for g in range(groups):
                    finalize(home(step), g)

    if relay:
        @pl.when(place == 0)
        def _():
            for i in range(2):
                out_hop(0, across[i], i).wait_recv()
                out_next(i).start()

    def m_arrival(source, r):
        there = got.at[source, at_rows(r), :]
        return pltpu.make_async_remote_copy(
            src_ref=there, dst_ref=there, send_sem=m_send, recv_sem=m_recv.at[source, r],
            device_id={"mp": partner}, device_id_type=MESH)

    def q_arrival(r):
        there = sq_got.at[r, pl.ds(0, n_mp - 1)]
        return pltpu.make_async_remote_copy(
            src_ref=there, dst_ref=there, send_sem=q_send, recv_sem=q_recv.at[r],
            device_id={"mp": partner}, device_id_type=MESH)

    sources = [me, partner] + [lax.rem(chip + t, chips) * 2 + lax.rem(core + s, 2) for t in range(1, chips) for s in (0, 1)]

    for r in range(parts):
        q_arrival(r).wait_recv()
        total = sq_got[r, 0]
        for source in range(1, n_mp):
            total += sq_got[r, source]
        scale = lax.rsqrt(total * (1.0 / (n_mp * width)) + 1e-06)
        scale = jnp.broadcast_to(scale, (8, rows)).T[:, 0:1]
        span = slice(r * rows, (r + 1) * rows)
        for i, source in enumerate(sources):
            if i > 0:
                m_arrival(source, r).wait_recv()
            out[span, columns(source)] = (got[source, span, :].astype(F32) * scale * gain[:, columns(source)]).astype(BF16)

    def sent(ref, sem):
        pltpu.make_async_remote_copy(
            src_ref=ref, dst_ref=ref, send_sem=sem, recv_sem=own_sem,
            device_id={"mp": partner}, device_id_type=MESH).wait_send()

    for step in range(1, chips):
        sent(tokens, y_send.at[step - 1])
        sent(x.at[:, columns(0)], d_send.at[step - 1])
    sent(tokens, p_send)
    sent(sq_out.at[pl.ds(0, chunks - parts)], q_send)
    sent(moved.at[pl.ds(0, seq_rows - own_rows), :], m_send)
    if n_seq > 1:
        pl.when(place < n_seq - 1)(lambda: sent(state_out, s_send))
    if relay:
        pl.when(place == 0)(lambda: sent(hop_out, hop_send))
        pl.when(place == 1)(lambda: sent(hop_in, hop_send))


def in_hbm(a):
    return a if a.size == 1 else pltpu.with_memory_space_constraint(a, pltpu.HBM)


def body(n_mp, n_seq, tokens, w_query, w_key, w_value, w_gate, decay_exponent, forget, norm_gain):
    seq_rows, width = tokens.shape
    features = w_query.shape[0]
    heads = decay_exponent.shape[0]
    own_rows = seq_rows // n_mp
    rows = 256 if own_rows % 256 == 0 else own_rows
    chunks, parts = seq_rows // rows, own_rows // rows
    groups = 2 if heads % 2 == 0 else 1
    hbm = pl.BlockSpec(memory_space=pltpu.HBM)
    dma = pltpu.SemaphoreType.DMA
    chips = n_mp // 2
    return pl.pallas_call(
        functools.partial(kernel, n_mp, n_seq, heads, rows, groups),
        out_shape=pltpu.VMEM((own_rows, features), BF16),
        in_specs=[hbm] * 8,
        out_specs=pl.BlockSpec(memory_space=pltpu.VMEM),
        scratch_shapes=[
            pltpu.VMEM((seq_rows, features), BF16),
            pltpu.VMEM((4, features, width), BF16),
            pltpu.VMEM((1, heads), jnp.int32),
            pltpu.VMEM((heads, seq_rows), F32),
            pltpu.VMEM((1, features), F32),
            pltpu.VMEM((chunks * heads, rows), F32),
            pltpu.VMEM((chunks, heads, rows), F32),
            pltpu.VMEM((chunks, rows, heads), F32),
            pltpu.VMEM((4, 4, rows, width), F32),
            pltpu.VMEM((seq_rows, width), F32),
            pltpu.VMEM((seq_rows, width), BF16),
            pltpu.VMEM((seq_rows, width), F32),
            pltpu.VMEM((seq_rows, width), BF16),
            pltpu.VMEM((n_mp, own_rows, width), BF16),
            pltpu.VMEM((chunks, 1, rows), F32),
            pltpu.VMEM((parts, n_mp, 1, rows), F32),
            pltpu.VMEM((heads, DH, DH), F32),
            pltpu.VMEM((heads, DH, DH), BF16),
            pltpu.VMEM((heads, DH, DH), BF16),
            pltpu.VMEM((heads, DH, DH), BF16),
            pltpu.VMEM((heads, DH, DH), BF16),
            pltpu.VMEM((heads, 128), F32),
            pltpu.VMEM((rows, width), BF16),
            pltpu.VMEM((2, rows - 16, width // groups), BF16),
            dma,
            dma((3,)),
            dma,
            dma((chips - 1,)),
            dma((chunks, chips - 1)),
            dma,
            dma((chunks // 2,)),
            dma((chips - 1,)),
            dma((chunks, chips - 1)),
            dma,
            dma((groups,)),
            dma,
            dma((n_mp, parts)),
            dma,
            dma((parts,)),
            dma,
            dma((2,)),
            pltpu.SemaphoreType.REGULAR,
        ],
        compiler_params=pltpu.CompilerParams(
            collective_id=0, has_side_effects=True, vmem_limit_bytes=56 * 1024 * 1024
        ),
    )(*(in_hbm(a) for a in (tokens, w_query, w_key, w_value, w_gate, decay_exponent[None, :], forget.T, norm_gain[None, :])))


def solution(mesh):
    placed = (
        P(("dp", "seq"), "mp"),
        P(None, "mp"),
        P(None, "mp"),
        P(None, "mp"),
        P(None, "mp"),
        P("mp"),
        P(("dp", "seq"), "mp"),
        P(),
    )
    return jax.shard_map(
        functools.partial(body, mesh.shape["mp"], mesh.shape["seq"]),
        mesh=mesh,
        in_specs=placed,
        out_specs=P(("dp", "seq", "mp"), None),
        check_vma=False,
    )
```

```python
import functools

import jax
import jax.numpy as jnp
from jax import lax
from jax.experimental import pallas as pl
from jax.experimental.pallas import tpu as pltpu
from jax.sharding import PartitionSpec as P

DH = 128
MESH = pl.DeviceIdType.MESH
F32 = jnp.float32
BF16 = jnp.bfloat16


def contract(a, b, dims):
    return lax.dot_general(a, b, ((dims[0], dims[1]), ((), ())), preferred_element_type=F32)


def kernel(
    n_mp, n_seq, heads, rows, groups,
    tokens, wq, wk, wv, wg, exponent_in, forget_in, gain_in, out,
    x, w, exponent, forget, gain, decays, summed, by_rows, partial, local_out, q_in, gates, moved, got, sq_out, sq_got,
    state, held, enter, state_out, state_got, offset, hop_in, hop_out,
    weight_sem, small_sem, own_sem, y_send, y_recv, p_send, p_recv, d_send, d_recv, s_send, s_recv, m_send, m_recv, q_send, q_recv, hop_send, hop_recv, ready,
):
    me = lax.axis_index("mp")
    place = lax.axis_index("seq")
    chips = n_mp // 2
    chip, core = me // 2, me % 2
    partner = chip * 2 + (1 - core)
    seq_rows, width = tokens.shape
    chunks = seq_rows // rows
    own_rows = seq_rows // n_mp
    parts = own_rows // rows
    head_width = width // heads
    group_heads = heads // groups
    group_width = width // groups
    ahead = partial.shape[0]
    relay = n_seq == 2 and chips == 2
    hop_chunk = 3 if chunks > 4 else chunks - 1
    across = [lax.rem(chip + 1, chips) * 2 + core, lax.rem(chip + 1, chips) * 2 + (1 - core)]

    barrier = pltpu.get_barrier_semaphore()
    greeted = [lax.rem(chip + t, chips) * 2 + core for t in range(1, chips)] + [partner]
    for there in greeted:
        pl.semaphore_signal(barrier, inc=1, device_id={"mp": there}, device_id_type=MESH)

    across_place = [{"seq": 1 - place}] + [{"mp": there, "seq": 1 - place} for there in across]

    if relay:
        @pl.when(place == 0)
        def _():
            for there in across_place:
                pl.semaphore_signal(barrier, inc=1, device_id=there, device_id_type=MESH)
    else:
        @pl.when(place > 0)
        def _():
            pl.semaphore_signal(barrier, inc=1, device_id={"seq": place - 1}, device_id_type=MESH)

        @pl.when(place < n_seq - 1)
        def _():
            pl.semaphore_signal(barrier, inc=1, device_id={"seq": place + 1}, device_id_type=MESH)

    weights = [pltpu.make_async_copy(src, w.at[i], weight_sem) for i, src in enumerate((wk, wv, wq, wg))]
    small = [
        pltpu.make_async_copy(src, dst, small_sem.at[i])
        for i, (src, dst) in enumerate(((exponent_in, exponent), (forget_in, forget), (gain_in, gain)))
    ]

    def relative(source, to):
        return lax.rem(source - to + n_mp, n_mp) - 1

    def columns(block):
        return pl.ds(pl.multiple_of(block * width, width), width)

    def at_rows(c):
        return pl.ds(pl.multiple_of(c * rows, rows), rows)

    def own_copy():
        return pltpu.make_async_copy(tokens, x.at[:, columns(me)], own_sem)

    def far(step):
        return lax.rem(chip + step, chips) * 2 + core

    def back(step):
        return lax.rem(chip + chips - step, chips) * 2 + core

    def back_other(step):
        return lax.rem(chip + chips - step, chips) * 2 + (1 - core)

    def y_copy(c, step):
        return pltpu.make_async_remote_copy(
            src_ref=tokens.at[at_rows(c), :], dst_ref=x.at[at_rows(c), columns(me)],
            send_sem=y_send.at[step - 1], recv_sem=y_recv.at[c, step - 1],
            device_id={"mp": far(step)}, device_id_type=MESH)

    def y_arrival(c, step):
        return pltpu.make_async_remote_copy(
            src_ref=tokens.at[at_rows(c), :], dst_ref=x.at[at_rows(c), columns(back(step))],
            send_sem=y_send.at[step - 1], recv_sem=y_recv.at[c, step - 1],
            device_id={"mp": far(step)}, device_id_type=MESH)

    def at_pair(i):
        return pl.ds(pl.multiple_of(i * 2 * rows, 2 * rows), 2 * rows)

    def p_copy(i):
        return pltpu.make_async_remote_copy(
            src_ref=tokens.at[at_pair(i), :], dst_ref=x.at[at_pair(i), columns(me)],
            send_sem=p_send, recv_sem=p_recv.at[i],
            device_id={"mp": partner}, device_id_type=MESH)

    def p_arrival(i):
        there = x.at[at_pair(i), columns(partner)]
        return pltpu.make_async_remote_copy(
            src_ref=there, dst_ref=there, send_sem=p_send, recv_sem=p_recv.at[i],
            device_id={"mp": partner}, device_id_type=MESH)

    def d_copy(c, step):
        there = x.at[at_rows(c), columns(back(step))]
        return pltpu.make_async_remote_copy(
            src_ref=there, dst_ref=there, send_sem=d_send.at[step - 1], recv_sem=d_recv.at[c, step - 1],
            device_id={"mp": partner}, device_id_type=MESH)

    def d_arrival(c, step):
        there = x.at[at_rows(c), columns(back_other(step))]
        return pltpu.make_async_remote_copy(
            src_ref=there, dst_ref=there, send_sem=d_send.at[step - 1], recv_sem=d_recv.at[c, step - 1],
            device_id={"mp": partner}, device_id_type=MESH)

    kept_rows = rows - hop_in.shape[0]
    hop_span = pl.ds(hop_chunk * rows + kept_rows, rows - kept_rows)

    def y_rest():
        span = pl.ds(hop_chunk * rows, kept_rows)
        return pltpu.make_async_remote_copy(
            src_ref=tokens.at[span, :], dst_ref=x.at[span, columns(me)],
            send_sem=y_send.at[0], recv_sem=y_recv.at[hop_chunk, 0],
            device_id={"mp": across[0]}, device_id_type=MESH)

    def in_hop():
        return pltpu.make_async_remote_copy(
            src_ref=tokens.at[hop_span, :], dst_ref=hop_in,
            send_sem=y_send.at[0], recv_sem=hop_recv.at[0],
            device_id={"mp": across[0], "seq": 1}, device_id_type=MESH)

    def in_next():
        return pltpu.make_async_remote_copy(
            src_ref=hop_in, dst_ref=x.at[hop_span, columns(across[0])],
            send_sem=hop_send, recv_sem=y_recv.at[hop_chunk, 0],
            device_id={"seq": 0}, device_id_type=MESH)

    hop_rows = hop_out.shape[1]

    def out_hop(block, to, i):
        return pltpu.make_async_remote_copy(
            src_ref=moved.at[pl.ds(pl.multiple_of(block * rows, rows), hop_rows), pl.ds(0, group_width)],
            dst_ref=hop_out.at[i], send_sem=m_send, recv_sem=hop_recv.at[i],
            device_id={"mp": to, "seq": 0}, device_id_type=MESH)

    def out_rest(block, to):
        left = rows - hop_rows
        return pltpu.make_async_remote_copy(
            src_ref=moved.at[pl.ds(pl.multiple_of(block * rows + hop_rows, 16), left), pl.ds(0, group_width)],
            dst_ref=got.at[me, pl.ds(hop_rows, left), pl.ds(0, group_width)],
            send_sem=m_send, recv_sem=m_recv.at[relative(me, to), 0], device_id={"mp": to}, device_id_type=MESH)

    def out_next(i):
        return pltpu.make_async_remote_copy(
            src_ref=hop_out.at[i], dst_ref=got.at[across[i], pl.ds(0, hop_rows), pl.ds(0, group_width)],
            send_sem=hop_send, recv_sem=m_recv.at[relative(across[i], me), 0],
            device_id={"seq": 1}, device_id_type=MESH)

    for copy in small:
        copy.start()
    own_copy().start()
    for copy in weights:
        copy.start()

    if relay:
        neighbours = place * len(across_place)
    else:
        neighbours = jnp.minimum(place, 1) + jnp.minimum(n_seq - 1 - place, 1)
    pl.semaphore_wait(barrier, len(greeted) + neighbours)

    @pl.loop(0, chunks)
    def _(c):
        for step in range(1, chips):
            if relay:
                whole = jnp.logical_or(place > 0, c != hop_chunk)
                pl.when(whole)(lambda: y_copy(c, step).start())
                pl.when(jnp.logical_not(whole))(lambda: y_rest().start())
            else:
                y_copy(c, step).start()
        pl.when(lax.rem(c, 2) == 0)(lambda: p_copy(c // 2).start())

    if relay:
        @pl.when(place == 1)
        def _():
            for there in across_place:
                pl.semaphore_signal(ready, inc=1, device_id=there, device_id_type=MESH)

    state[...] = jnp.zeros_like(state)
    offset[...] = jnp.zeros_like(offset)
    enter[...] = jnp.zeros_like(enter)

    later = lax.broadcasted_iota(jnp.int32, (rows, rows), 0)
    earlier = lax.broadcasted_iota(jnp.int32, (rows, rows), 1)
    causal = later >= earlier
    summing = (later <= earlier).astype(F32)
    exact = lax.Precision.HIGHEST
    ones = jnp.ones((8, head_width), BF16)

    for copy in small:
        copy.wait()
    spread = jnp.broadcast_to(exponent[...].astype(F32), (heads, heads))
    diagonal = lax.broadcasted_iota(jnp.int32, (heads, heads), 0) == lax.broadcasted_iota(jnp.int32, (heads, heads), 1)
    column = jnp.sum(jnp.where(diagonal, spread, 0.0), axis=1, keepdims=True)
    rate = jnp.log1p(-jnp.exp2(-column))
    for c in range(chunks):
        decays[c * heads : (c + 1) * heads, :] = rate - forget[:, c * rows : (c + 1) * rows]
    every = jnp.dot(decays[...], summing, precision=exact, preferred_element_type=F32)
    turned = every.T
    for c in range(chunks):
        summed[c] = every[c * heads : (c + 1) * heads, :]
        by_rows[c] = turned[:, c * heads : (c + 1) * heads]

    def near(c):
        pl.when(lax.rem(c, 2) == 0)(lambda: p_arrival(c // 2).wait_recv())
        own_side = pl.ds(pl.multiple_of(chip * 2 * width, 2 * width), 2 * width)
        piece = x[at_rows(c), own_side]
        slot = lax.rem(c, ahead)
        for i in range(4):
            partial[slot, i] = jnp.dot(piece, w[i, own_side, :], preferred_element_type=F32)

    if relay:
        @pl.when(place == 0)
        def _():
            pl.semaphore_wait(ready, len(across_place))
            in_hop().start()

    own_copy().wait()
    pltpu.make_async_copy(w, w, weight_sem).wait()
    pl.loop(0, ahead)(near)

    def s_copy(g):
        part = pl.ds(g * group_heads, group_heads)
        return pltpu.make_async_remote_copy(
            src_ref=state_out.at[part], dst_ref=state_got.at[part], send_sem=s_send, recv_sem=s_recv.at[g],
            device_id={"seq": lax.rem(place + 1, n_seq)}, device_id_type=MESH)

    def group_columns(g):
        return pl.ds(g * group_width, group_width)

    def m_copy(block, g):
        to, r = block // parts, lax.rem(block, parts)
        return pltpu.make_async_remote_copy(
            src_ref=moved.at[at_rows(block), group_columns(g)], dst_ref=got.at[me, at_rows(r), group_columns(g)],
            send_sem=m_send, recv_sem=m_recv.at[relative(me, to), r],
            device_id={"mp": to}, device_id_type=MESH)

    def q_copy(block):
        to, r = block // parts, lax.rem(block, parts)
        return pltpu.make_async_remote_copy(
            src_ref=sq_out.at[block], dst_ref=sq_got.at[r, me],
            send_sem=q_send, recv_sem=q_recv.at[r],
            device_id={"mp": to}, device_id_type=MESH)

    def finalize(block, g):
        here = at_rows(block)
        to, r = block // parts, lax.rem(block, parts)
        square = jnp.zeros((rows, head_width), F32)
        for h in range(g * group_heads, (g + 1) * group_heads):
            part = slice(h * head_width, (h + 1) * head_width)
            whole = local_out[here, part] + jnp.dot(q_in[here, part], enter[h], preferred_element_type=F32)
            kept = whole.astype(BF16).astype(F32)
            moved[here, part] = (gates[here, part] * kept).astype(BF16)
            square += kept * kept
        high = square.astype(BF16)
        low = (square - high.astype(F32)).astype(BF16)
        total = (contract(ones, high, ((1,), (1,))) + contract(ones, low, ((1,), (1,))))[0:1, :]
        if g > 0:
            total = total + sq_out[block]
        sq_out[block] = total

        @pl.when(to != me)
        def _():
            if g == groups - 1:
                q_copy(block).start()
            if relay and g == 0:
                detour = jnp.logical_and(jnp.logical_and(place == 1, r == 0), to // 2 != chip)

                @pl.when(detour)
                def _():
                    out_hop(block, to, lax.rem(core + to, 2)).start()
                    out_rest(block, to).start()

                pl.when(jnp.logical_not(detour))(lambda: m_copy(block, g).start())
            else:
                m_copy(block, g).start()

        @pl.when(to == me)
        def _():
            part = slice(g * group_width, (g + 1) * group_width)
            got[me, at_rows(r), part] = moved[here, part]
            if g == groups - 1:
                sq_got[r, me] = total

    far_steps = (n_mp - 2) * parts

    def away(step):
        o = lax.rem(step, n_mp - 2)
        return (lax.rem(chip + o // 2 + 1, chips) * 2 + lax.rem(core + o, 2)) * parts + step // (n_mp - 2)

    def home(step):
        return (chip * 2 + lax.rem(core + 1 + step, 2)) * parts + step // 2

    def enter_state(g):
        part = slice(g * group_heads, (g + 1) * group_heads)
        s_copy(g).wait_recv()
        enter[part] = state_got[part]

    def ready_far(g, low, high):
        @pl.loop(0, far_steps)
        def _(step):
            block = away(lax.rem(step + 2, far_steps) if g == 0 else step)
            pl.when(jnp.logical_and(block >= low, block < high))(lambda: finalize(block, g))

    @pl.loop(0, chunks)
    def _(c):
        here = at_rows(c)
        slot = lax.rem(c, ahead)
        running, by_row = summed[c], by_rows[c]
        last = running[:, rows - 1 :]
        before = offset[...]

        if relay:
            @pl.when(jnp.logical_and(place == 1, c == 1))
            def _():
                in_hop().wait_recv()
                in_next().start()

            @pl.when(jnp.logical_and(place == 1, c == chunks - 1))
            def _():
                ready_far(0, chunks - 2, chunks - 1)
                for g in range(1, groups):
                    enter_state(g)
                    ready_far(g, 0, chunks - 1)

        for step in range(1, chips):
            y_arrival(c, step).wait_recv()
            d_copy(c, step).start()
        for step in range(1, chips):
            piece = x[here, columns(back(step))]
            for i in range(4):
                partial[slot, i] += jnp.dot(piece, w[i, columns(back(step)), :], preferred_element_type=F32)

        @pl.when(jnp.logical_and(place == 0, c > 0))
        def _():
            for g in range(groups):
                finalize(c - 1, g)

        for step in range(1, chips):
            d_arrival(c, step).wait_recv()

        if relay:
            @pl.when(jnp.logical_and(place == 1, c == chunks - 2))
            def _():
                enter_state(0)
                ready_far(0, 0, chunks - 2)

        def project(i):
            total = partial[slot, i]
            for step in range(1, chips):
                total += jnp.dot(
                    x[here, columns(back_other(step))], w[i, columns(back_other(step)), :],
                    preferred_element_type=F32)
            return total

        key = (project(0) * DH ** (-0.5)).astype(BF16)
        value = project(1).astype(BF16)
        for h in range(heads):
            part = slice(h * head_width, (h + 1) * head_width)
            k, v = key[:, part], value[:, part]
            end = last[h : h + 1, :]
            grown = state[h]
            held[h] = grown.astype(BF16)
            faded = (k.astype(F32) * jnp.exp(end - by_row[:, h : h + 1])).astype(BF16)
            state[h] = jnp.exp(end) * grown + contract(faded, v, ((0,), (0,)))

        @pl.when(jnp.logical_and(place == 0, c == chunks - 1))
        def _():
            state_out[...] = state[...].astype(BF16)
            if n_seq > 1:
                for g in range(groups):
                    s_copy(g).start()

        query = project(2).astype(BF16)
        for h in range(heads):
            part = slice(h * head_width, (h + 1) * head_width)
            q, k, v = query[:, part], key[:, part], value[:, part]
            col = by_row[:, h : h + 1]
            mask = jnp.exp(jnp.where(causal, col - running[h : h + 1, :], -1e30))
            scores = (contract(q, k, ((1,), (1,))) * mask).astype(BF16)
            qf = q.astype(F32)
            carried = jnp.dot((qf * jnp.exp(col)).astype(BF16), held[h], preferred_element_type=F32)
            local_out[here, part] = jnp.dot(scores, v, preferred_element_type=F32) + carried
            q_in[here, part] = (qf * jnp.exp(col + before[h : h + 1, 0:1])).astype(BF16)
        offset[...] = before + last
        gate = project(3).astype(BF16).astype(F32)
        gates[here, :] = gate / (1.0 + jnp.exp(-gate))

        pl.when(c < chunks - ahead)(lambda: near(c + ahead))

    @pl.when(place == 0)
    def _():
        for g in range(groups):
            finalize(chunks - 1, g)

    if n_seq > 1:
        @pl.when(place > 0)
        def _():
            for g in range(groups):
                if relay:
                    pl.when((chunks - 1) // parts // 2 != chip)(lambda: finalize(chunks - 1, g))
                    continue
                enter_state(g)
                if n_seq > 2:
                    @pl.when(place < n_seq - 1)
                    def _():
                        for h in range(g * group_heads, (g + 1) * group_heads):
                            total = jnp.exp(offset[h : h + 1, 0:1])
                            state_out[h] = (total * enter[h].astype(F32) + state[h]).astype(BF16)
                        s_copy(g).start()

                pl.loop(0, far_steps)(lambda step: finalize(away(step), g))

            @pl.loop(0, 2 * parts)
            def _(step):
                for g in range(groups):
                    finalize(home(step), g)

    if relay:
        @pl.when(place == 0)
        def _():
            for i in range(2):
                out_hop(0, across[i], i).wait_recv()
                out_next(i).start()

    def m_arrival(source, r):
        there = got.at[source, at_rows(r), :]
        return pltpu.make_async_remote_copy(
            src_ref=there, dst_ref=there, send_sem=m_send, recv_sem=m_recv.at[relative(source, me), r],
            device_id={"mp": partner}, device_id_type=MESH)

    def q_arrival(r):
        there = sq_got.at[r, pl.ds(0, n_mp - 1)]
        return pltpu.make_async_remote_copy(
            src_ref=there, dst_ref=there, send_sem=q_send, recv_sem=q_recv.at[r],
            device_id={"mp": partner}, device_id_type=MESH)

    sources = [me, partner] + [lax.rem(chip + t, chips) * 2 + lax.rem(core + s, 2) for t in range(1, chips) for s in (0, 1)]

    for r in range(parts):
        q_arrival(r).wait_recv()
        total = sq_got[r, 0]
        for source in range(1, n_mp):
            total += sq_got[r, source]
        scale = lax.rsqrt(total * (1.0 / (n_mp * width)) + 1e-06)
        scale = jnp.broadcast_to(scale, (8, rows)).T[:, 0:1]
        span = slice(r * rows, (r + 1) * rows)
        for i, source in enumerate(sources):
            if i > 0:
                m_arrival(source, r).wait_recv()
            out[span, columns(source)] = (got[source, span, :].astype(F32) * scale * gain[:, columns(source)]).astype(BF16)

    def sent(ref, sem):
        pltpu.make_async_remote_copy(
            src_ref=ref, dst_ref=ref, send_sem=sem, recv_sem=own_sem,
            device_id={"mp": partner}, device_id_type=MESH).wait_send()

    for step in range(1, chips):
        sent(tokens, y_send.at[step - 1])
        sent(x.at[:, columns(0)], d_send.at[step - 1])
    sent(tokens, p_send)
    sent(sq_out.at[pl.ds(0, chunks - parts)], q_send)
    sent(moved.at[pl.ds(0, seq_rows - own_rows), :], m_send)
    if n_seq > 1:
        pl.when(place < n_seq - 1)(lambda: sent(state_out, s_send))
    if relay:
        pl.when(place == 0)(lambda: sent(hop_out, hop_send))
        pl.when(place == 1)(lambda: sent(hop_in, hop_send))


def in_hbm(a):
    return a if a.size == 1 else pltpu.with_memory_space_constraint(a, pltpu.HBM)


def body(n_mp, n_seq, tokens, w_query, w_key, w_value, w_gate, decay_exponent, forget, norm_gain):
    seq_rows, width = tokens.shape
    features = w_query.shape[0]
    heads = decay_exponent.shape[0]
    own_rows = seq_rows // n_mp
    rows = 256 if own_rows % 256 == 0 else own_rows
    chunks, parts = seq_rows // rows, own_rows // rows
    groups = 2 if heads % 2 == 0 else 1
    hbm = pl.BlockSpec(memory_space=pltpu.HBM)
    dma = pltpu.SemaphoreType.DMA
    chips = n_mp // 2
    return pl.pallas_call(
        functools.partial(kernel, n_mp, n_seq, heads, rows, groups),
        out_shape=pltpu.VMEM((own_rows, features), BF16),
        in_specs=[hbm] * 8,
        out_specs=pl.BlockSpec(memory_space=pltpu.VMEM),
        scratch_shapes=[
            pltpu.VMEM((seq_rows, features), BF16),
            pltpu.VMEM((4, features, width), BF16),
            pltpu.VMEM((1, heads), jnp.int32),
            pltpu.VMEM((heads, seq_rows), F32),
            pltpu.VMEM((1, features), F32),
            pltpu.VMEM((chunks * heads, rows), F32),
            pltpu.VMEM((chunks, heads, rows), F32),
            pltpu.VMEM((chunks, rows, heads), F32),
            pltpu.VMEM((4, 4, rows, width), F32),
            pltpu.VMEM((seq_rows, width), F32),
            pltpu.VMEM((seq_rows, width), BF16),
            pltpu.VMEM((seq_rows, width), F32),
            pltpu.VMEM((seq_rows, width), BF16),
            pltpu.VMEM((n_mp, own_rows, width), BF16),
            pltpu.VMEM((chunks, 1, rows), F32),
            pltpu.VMEM((parts, n_mp, 1, rows), F32),
            pltpu.VMEM((heads, DH, DH), F32),
            pltpu.VMEM((heads, DH, DH), BF16),
            pltpu.VMEM((heads, DH, DH), BF16),
            pltpu.VMEM((heads, DH, DH), BF16),
            pltpu.VMEM((heads, DH, DH), BF16),
            pltpu.VMEM((heads, 128), F32),
            pltpu.VMEM((rows - 64, width), BF16),
            pltpu.VMEM((2, rows - 80, width // groups), BF16),
            dma,
            dma((3,)),
            dma,
            dma((chips - 1,)),
            dma((chunks, chips - 1)),
            dma,
            dma((chunks // 2,)),
            dma((chips - 1,)),
            dma((chunks, chips - 1)),
            dma,
            dma((groups,)),
            dma,
            dma((n_mp - 1, parts)),
            dma,
            dma((parts,)),
            dma,
            dma((2,)),
            pltpu.SemaphoreType.REGULAR,
        ],
        compiler_params=pltpu.CompilerParams(
            collective_id=0, has_side_effects=True, vmem_limit_bytes=56 * 1024 * 1024
        ),
    )(*(in_hbm(a) for a in (tokens, w_query, w_key, w_value, w_gate, decay_exponent[None, :], forget.T, norm_gain[None, :])))


def solution(mesh):
    placed = (
        P(("dp", "seq"), "mp"),
        P(None, "mp"),
        P(None, "mp"),
        P(None, "mp"),
        P(None, "mp"),
        P("mp"),
        P(("dp", "seq"), "mp"),
        P(),
    )
    return jax.shard_map(
        functools.partial(body, mesh.shape["mp"], mesh.shape["seq"]),
        mesh=mesh,
        in_specs=placed,
        out_specs=P(("dp", "seq", "mp"), None),
        check_vma=False,
    )
```

```python
import functools

import jax
import jax.numpy as jnp
from jax import lax
from jax.experimental import pallas as pl
from jax.experimental.pallas import tpu as pltpu
from jax.sharding import PartitionSpec as P

DH = 128
MESH = pl.DeviceIdType.MESH
F32 = jnp.float32
BF16 = jnp.bfloat16


def contract(a, b, dims):
    return lax.dot_general(a, b, ((dims[0], dims[1]), ((), ())), preferred_element_type=F32)


def token_units(n_mp, n_seq, chunks):
    if n_seq == 2 and n_mp == 4 and chunks > 7:
        return [(0, 1), (1, 2), (3, 1), (4, 2)] + [(c, 1) for c in range(6, chunks)]
    return None


def kernel(
    n_mp, n_seq, heads, rows, groups,
    tokens, wq, wk, wv, wg, exponent_in, forget_in, gain_in, out,
    x, w, exponent, forget, gain, decays, summed, by_rows, partial, local_out, q_in, gates, moved, got, sq_out, sq_got,
    state, held, enter, state_out, state_got, offset, hop_in, hop_out,
    weight_sem, small_sem, own_sem, y_send, y_recv, p_send, p_recv, d_send, d_recv, s_send, s_recv, m_send, m_recv, q_send, q_recv, hop_send, hop_recv, ready,
):
    me = lax.axis_index("mp")
    place = lax.axis_index("seq")
    chips = n_mp // 2
    chip, core = me // 2, me % 2
    partner = chip * 2 + (1 - core)
    seq_rows, width = tokens.shape
    chunks = seq_rows // rows
    own_rows = seq_rows // n_mp
    parts = own_rows // rows
    head_width = width // heads
    group_heads = heads // groups
    group_width = width // groups
    ahead = partial.shape[0]
    relay = n_seq == 2 and chips == 2
    hop_chunk = 3 if chunks > 4 else chunks - 1
    across = [lax.rem(chip + 1, chips) * 2 + core, lax.rem(chip + 1, chips) * 2 + (1 - core)]

    barrier = pltpu.get_barrier_semaphore()
    greeted = [lax.rem(chip + t, chips) * 2 + core for t in range(1, chips)] + [partner]
    for there in greeted:
        pl.semaphore_signal(barrier, inc=1, device_id={"mp": there}, device_id_type=MESH)

    across_place = [{"seq": 1 - place}] + [{"mp": there, "seq": 1 - place} for there in across]

    if relay:
        @pl.when(place == 0)
        def _():
            for there in across_place:
                pl.semaphore_signal(barrier, inc=1, device_id=there, device_id_type=MESH)
    else:
        @pl.when(place > 0)
        def _():
            pl.semaphore_signal(barrier, inc=1, device_id={"seq": place - 1}, device_id_type=MESH)

        @pl.when(place < n_seq - 1)
        def _():
            pl.semaphore_signal(barrier, inc=1, device_id={"seq": place + 1}, device_id_type=MESH)

    weights = [pltpu.make_async_copy(src, w.at[i], weight_sem) for i, src in enumerate((wk, wv, wq, wg))]
    small = [
        pltpu.make_async_copy(src, dst, small_sem.at[i])
        for i, (src, dst) in enumerate(((exponent_in, exponent), (forget_in, forget), (gain_in, gain)))
    ]

    def relative(source, to):
        return lax.rem(source - to + n_mp, n_mp) - 1

    def columns(block):
        return pl.ds(pl.multiple_of(block * width, width), width)

    def at_rows(c):
        return pl.ds(pl.multiple_of(c * rows, rows), rows)

    def own_copy():
        return pltpu.make_async_copy(tokens, x.at[:, columns(me)], own_sem)

    def far(step):
        return lax.rem(chip + step, chips) * 2 + core

    def back(step):
        return lax.rem(chip + chips - step, chips) * 2 + core

    def back_other(step):
        return lax.rem(chip + chips - step, chips) * 2 + (1 - core)

    units = token_units(n_mp, n_seq, chunks)
    unit_of_hop = hop_chunk if units is None else [first for first, _ in units].index(hop_chunk)

    def unit_rows(i):
        return at_rows(i) if units is None else pl.ds(units[i][0] * rows, units[i][1] * rows)

    def y_copy(c, step):
        return pltpu.make_async_remote_copy(
            src_ref=tokens.at[unit_rows(c), :], dst_ref=x.at[unit_rows(c), columns(me)],
            send_sem=y_send.at[step - 1], recv_sem=y_recv.at[c, step - 1],
            device_id={"mp": far(step)}, device_id_type=MESH)

    def y_arrival(c, step):
        return pltpu.make_async_remote_copy(
            src_ref=tokens.at[unit_rows(c), :], dst_ref=x.at[unit_rows(c), columns(back(step))],
            send_sem=y_send.at[step - 1], recv_sem=y_recv.at[c, step - 1],
            device_id={"mp": far(step)}, device_id_type=MESH)

    def at_pair(i):
        return (pl.ds(0, 2 * rows), pl.ds(2 * rows, seq_rows - 2 * rows))[i]

    def p_copy(i):
        return pltpu.make_async_remote_copy(
            src_ref=tokens.at[at_pair(i), :], dst_ref=x.at[at_pair(i), columns(me)],
            send_sem=p_send, recv_sem=p_recv.at[i],
            device_id={"mp": partner}, device_id_type=MESH)

    def p_arrival(i):
        there = x.at[at_pair(i), columns(partner)]
        return pltpu.make_async_remote_copy(
            src_ref=there, dst_ref=there, send_sem=p_send, recv_sem=p_recv.at[i],
            device_id={"mp": partner}, device_id_type=MESH)

    def d_copy(c, step):
        there = x.at[unit_rows(c), columns(back(step))]
        return pltpu.make_async_remote_copy(
            src_ref=there, dst_ref=there, send_sem=d_send.at[step - 1], recv_sem=d_recv.at[c, step - 1],
            device_id={"mp": partner}, device_id_type=MESH)

    def d_arrival(c, step):
        there = x.at[unit_rows(c), columns(back_other(step))]
        return pltpu.make_async_remote_copy(
            src_ref=there, dst_ref=there, send_sem=d_send.at[step - 1], recv_sem=d_recv.at[c, step - 1],
            device_id={"mp": partner}, device_id_type=MESH)

    kept_rows = rows - hop_in.shape[0]
    hop_span = pl.ds(hop_chunk * rows + kept_rows, rows - kept_rows)

    def y_rest():
        span = pl.ds(hop_chunk * rows, kept_rows)
        return pltpu.make_async_remote_copy(
            src_ref=tokens.at[span, :], dst_ref=x.at[span, columns(me)],
            send_sem=y_send.at[0], recv_sem=y_recv.at[unit_of_hop, 0],
            device_id={"mp": across[0]}, device_id_type=MESH)

    def in_hop():
        return pltpu.make_async_remote_copy(
            src_ref=tokens.at[hop_span, :], dst_ref=hop_in,
            send_sem=y_send.at[0], recv_sem=hop_recv.at[0],
            device_id={"mp": across[0], "seq": 1}, device_id_type=MESH)

    def in_next():
        return pltpu.make_async_remote_copy(
            src_ref=hop_in, dst_ref=x.at[hop_span, columns(across[0])],
            send_sem=hop_send, recv_sem=y_recv.at[unit_of_hop, 0],
            device_id={"seq": 0}, device_id_type=MESH)

    hop_rows = hop_out.shape[1]

    def out_hop(block, to, i):
        return pltpu.make_async_remote_copy(
            src_ref=moved.at[pl.ds(pl.multiple_of(block * rows, rows), hop_rows), pl.ds(0, group_width)],
            dst_ref=hop_out.at[i], send_sem=m_send, recv_sem=hop_recv.at[i],
            device_id={"mp": to, "seq": 0}, device_id_type=MESH)

    def out_rest(block, to):
        left = rows - hop_rows
        return pltpu.make_async_remote_copy(
            src_ref=moved.at[pl.ds(pl.multiple_of(block * rows + hop_rows, 16), left), pl.ds(0, group_width)],
            dst_ref=got.at[me, pl.ds(hop_rows, left), pl.ds(0, group_width)],
            send_sem=m_send, recv_sem=m_recv.at[relative(me, to), 0], device_id={"mp": to}, device_id_type=MESH)

    def out_next(i):
        return pltpu.make_async_remote_copy(
            src_ref=hop_out.at[i], dst_ref=got.at[across[i], pl.ds(0, hop_rows), pl.ds(0, group_width)],
            send_sem=hop_send, recv_sem=m_recv.at[relative(across[i], me), 0],
            device_id={"seq": 1}, device_id_type=MESH)

    for copy in small:
        copy.start()
    own_copy().start()
    for copy in weights:
        copy.start()

    if relay:
        neighbours = place * len(across_place)
    else:
        neighbours = jnp.minimum(place, 1) + jnp.minimum(n_seq - 1 - place, 1)
    pl.semaphore_wait(barrier, len(greeted) + neighbours)

    def send_unit(i, first):
        for step in range(1, chips):
            if relay and first == hop_chunk:
                pl.when(place > 0)(lambda: y_copy(i, step).start())
                pl.when(place == 0)(lambda: y_rest().start())
            else:
                y_copy(i, step).start()

    if units is None:
        for i in range(chunks):
            send_unit(i, i)
    else:
        for i, (first, _) in enumerate(units):
            send_unit(i, first)
            if i < 2:
                p_copy(i).start()
    if units is None:
        for i in range(2):
            p_copy(i).start()

    if relay:
        @pl.when(place == 1)
        def _():
            for there in across_place:
                pl.semaphore_signal(ready, inc=1, device_id=there, device_id_type=MESH)

    state[...] = jnp.zeros_like(state)
    offset[...] = jnp.zeros_like(offset)
    enter[...] = jnp.zeros_like(enter)

    later = lax.broadcasted_iota(jnp.int32, (rows, rows), 0)
    earlier = lax.broadcasted_iota(jnp.int32, (rows, rows), 1)
    causal = later >= earlier
    summing = (later <= earlier).astype(F32)
    exact = lax.Precision.HIGHEST
    ones = jnp.ones((8, head_width), BF16)

    for copy in small:
        copy.wait()
    spread = jnp.broadcast_to(exponent[...].astype(F32), (heads, heads))
    diagonal = lax.broadcasted_iota(jnp.int32, (heads, heads), 0) == lax.broadcasted_iota(jnp.int32, (heads, heads), 1)
    column = jnp.sum(jnp.where(diagonal, spread, 0.0), axis=1, keepdims=True)
    rate = jnp.log1p(-jnp.exp2(-column))
    for c in range(chunks):
        decays[c * heads : (c + 1) * heads, :] = rate - forget[:, c * rows : (c + 1) * rows]
    every = jnp.dot(decays[...], summing, precision=exact, preferred_element_type=F32)
    turned = every.T
    for c in range(chunks):
        summed[c] = every[c * heads : (c + 1) * heads, :]
        by_rows[c] = turned[:, c * heads : (c + 1) * heads]

    def near(c):
        pl.when(c == 0)(lambda: p_arrival(0).wait_recv())
        pl.when(c == 2)(lambda: p_arrival(1).wait_recv())
        own_side = pl.ds(pl.multiple_of(chip * 2 * width, 2 * width), 2 * width)
        piece = x[at_rows(c), own_side]
        slot = lax.rem(c, ahead)
        for i in range(4):
            partial[slot, i] = jnp.dot(piece, w[i, own_side, :], preferred_element_type=F32)

    if relay:
        @pl.when(place == 0)
        def _():
            pl.semaphore_wait(ready, len(across_place))
            in_hop().start()

    own_copy().wait()
    pltpu.make_async_copy(w, w, weight_sem).wait()
    pl.loop(0, ahead)(near)

    def s_copy(g):
        part = pl.ds(g * group_heads, group_heads)
        return pltpu.make_async_remote_copy(
            src_ref=state_out.at[part], dst_ref=state_got.at[part], send_sem=s_send, recv_sem=s_recv.at[g],
            device_id={"seq": lax.rem(place + 1, n_seq)}, device_id_type=MESH)

    def group_columns(g):
        return pl.ds(g * group_width, group_width)

    def m_copy(block, g):
        to, r = block // parts, lax.rem(block, parts)
        return pltpu.make_async_remote_copy(
            src_ref=moved.at[at_rows(block), group_columns(g)], dst_ref=got.at[me, at_rows(r), group_columns(g)],
            send_sem=m_send, recv_sem=m_recv.at[relative(me, to), r],
            device_id={"mp": to}, device_id_type=MESH)

    def q_copy(block):
        to, r = block // parts, lax.rem(block, parts)
        return pltpu.make_async_remote_copy(
            src_ref=sq_out.at[block], dst_ref=sq_got.at[r, me],
            send_sem=q_send, recv_sem=q_recv.at[r],
            device_id={"mp": to}, device_id_type=MESH)

    def finalize(block, g):
        here = at_rows(block)
        to, r = block // parts, lax.rem(block, parts)
        square = jnp.zeros((rows, head_width), F32)
        for h in range(g * group_heads, (g + 1) * group_heads):
            part = slice(h * head_width, (h + 1) * head_width)
            whole = local_out[here, part] + jnp.dot(q_in[here, part], enter[h], preferred_element_type=F32)
            kept = whole.astype(BF16).astype(F32)
            moved[here, part] = (gates[here, part] * kept).astype(BF16)
            square += kept * kept
        high = square.astype(BF16)
        low = (square - high.astype(F32)).astype(BF16)
        total = (contract(ones, high, ((1,), (1,))) + contract(ones, low, ((1,), (1,))))[0:1, :]
        if g > 0:
            total = total + sq_out[block]
        sq_out[block] = total

        @pl.when(to != me)
        def _():
            if g == groups - 1:
                q_copy(block).start()
            if relay and g == 0:
                detour = jnp.logical_and(jnp.logical_and(place == 1, r == 0), to // 2 != chip)

                @pl.when(detour)
                def _():
                    out_hop(block, to, lax.rem(core + to, 2)).start()
                    out_rest(block, to).start()

                pl.when(jnp.logical_not(detour))(lambda: m_copy(block, g).start())
            else:
                m_copy(block, g).start()

        @pl.when(to == me)
        def _():
            part = slice(g * group_width, (g + 1) * group_width)
            got[me, at_rows(r), part] = moved[here, part]
            if g == groups - 1:
                sq_got[r, me] = total

    far_steps = (n_mp - 2) * parts

    def away(step):
        o = lax.rem(step, n_mp - 2)
        return (lax.rem(chip + o // 2 + 1, chips) * 2 + lax.rem(core + o, 2)) * parts + step // (n_mp - 2)

    def home(step):
        return (chip * 2 + lax.rem(core + 1 + step, 2)) * parts + step // 2

    def enter_state(g):
        part = slice(g * group_heads, (g + 1) * group_heads)
        s_copy(g).wait_recv()
        enter[part] = state_got[part]

    def ready_far(g, low, high):
        @pl.loop(0, far_steps)
        def _(step):
            block = away(lax.rem(step + 2, far_steps) if g == 0 else step)
            pl.when(jnp.logical_and(block >= low, block < high))(lambda: finalize(block, g))

    @pl.loop(0, chunks)
    def _(c):
        here = at_rows(c)
        slot = lax.rem(c, ahead)
        running, by_row = summed[c], by_rows[c]
        last = running[:, rows - 1 :]
        before = offset[...]

        if relay:
            @pl.when(jnp.logical_and(place == 1, c == 1))
            def _():
                in_hop().wait_recv()
                in_next().start()

            @pl.when(jnp.logical_and(place == 1, c == chunks - 1))
            def _():
                ready_far(0, chunks - 2, chunks - 1)
                for g in range(1, groups):
                    enter_state(g)
                    ready_far(g, 0, chunks - 1)

        def forward(i):
            for step in range(1, chips):
                y_arrival(i, step).wait_recv()
                d_copy(i, step).start()

        def forwarded(i):
            for step in range(1, chips):
                d_arrival(i, step).wait_recv()

        def each_unit(act):
            if units is None:
                act(c)
            else:
                for i, (first, _) in enumerate(units):
                    pl.when(c == first)(functools.partial(act, i))

        each_unit(forward)
        for step in range(1, chips):
            piece = x[here, columns(back(step))]
            for i in range(4):
                partial[slot, i] += jnp.dot(piece, w[i, columns(back(step)), :], preferred_element_type=F32)

        @pl.when(jnp.logical_and(place == 0, c > 0))
        def _():
            for g in range(groups):
                finalize(c - 1, g)

        each_unit(forwarded)

        if relay:
            @pl.when(jnp.logical_and(place == 1, c == chunks - 2))
            def _():
                enter_state(0)
                ready_far(0, 0, chunks - 2)

        def project(i):
            total = partial[slot, i]
            for step in range(1, chips):
                total += jnp.dot(
                    x[here, columns(back_other(step))], w[i, columns(back_other(step)), :],
                    preferred_element_type=F32)
            return total

        key = (project(0) * DH ** (-0.5)).astype(BF16)
        value = project(1).astype(BF16)
        for h in range(heads):
            part = slice(h * head_width, (h + 1) * head_width)
            k, v = key[:, part], value[:, part]
            end = last[h : h + 1, :]
            grown = state[h]
            held[h] = grown.astype(BF16)
            faded = (k.astype(F32) * jnp.exp(end - by_row[:, h : h + 1])).astype(BF16)
            state[h] = jnp.exp(end) * grown + contract(faded, v, ((0,), (0,)))

        @pl.when(jnp.logical_and(place == 0, c == chunks - 1))
        def _():
            state_out[...] = state[...].astype(BF16)
            if n_seq > 1:
                for g in range(groups):
                    s_copy(g).start()

        query = project(2).astype(BF16)
        for h in range(heads):
            part = slice(h * head_width, (h + 1) * head_width)
            q, k, v = query[:, part], key[:, part], value[:, part]
            col = by_row[:, h : h + 1]
            mask = jnp.exp(jnp.where(causal, col - running[h : h + 1, :], -1e30))
            scores = (contract(q, k, ((1,), (1,))) * mask).astype(BF16)
            qf = q.astype(F32)
            carried = jnp.dot((qf * jnp.exp(col)).astype(BF16), held[h], preferred_element_type=F32)
            local_out[here, part] = jnp.dot(scores, v, preferred_element_type=F32) + carried
            q_in[here, part] = (qf * jnp.exp(col + before[h : h + 1, 0:1])).astype(BF16)
        offset[...] = before + last
        gate = project(3).astype(BF16).astype(F32)
        gates[here, :] = gate / (1.0 + jnp.exp(-gate))

        pl.when(c < chunks - ahead)(lambda: near(c + ahead))

    @pl.when(place == 0)
    def _():
        for g in range(groups):
            finalize(chunks - 1, g)

    if n_seq > 1:
        @pl.when(place > 0)
        def _():
            for g in range(groups):
                if relay:
                    pl.when((chunks - 1) // parts // 2 != chip)(lambda: finalize(chunks - 1, g))
                    continue
                enter_state(g)
                if n_seq > 2:
                    @pl.when(place < n_seq - 1)
                    def _():
                        for h in range(g * group_heads, (g + 1) * group_heads):
                            total = jnp.exp(offset[h : h + 1, 0:1])
                            state_out[h] = (total * enter[h].astype(F32) + state[h]).astype(BF16)
                        s_copy(g).start()

                pl.loop(0, far_steps)(lambda step: finalize(away(step), g))

            @pl.loop(0, 2 * parts)
            def _(step):
                for g in range(groups):
                    finalize(home(step), g)

    if relay:
        @pl.when(place == 0)
        def _():
            for i in range(2):
                out_hop(0, across[i], i).wait_recv()
                out_next(i).start()

    def m_arrival(source, r):
        there = got.at[source, at_rows(r), :]
        return pltpu.make_async_remote_copy(
            src_ref=there, dst_ref=there, send_sem=m_send, recv_sem=m_recv.at[relative(source, me), r],
            device_id={"mp": partner}, device_id_type=MESH)

    def q_arrival(r):
        there = sq_got.at[r, pl.ds(0, n_mp - 1)]
        return pltpu.make_async_remote_copy(
            src_ref=there, dst_ref=there, send_sem=q_send, recv_sem=q_recv.at[r],
            device_id={"mp": partner}, device_id_type=MESH)

    sources = [me, partner] + [lax.rem(chip + t, chips) * 2 + lax.rem(core + s, 2) for t in range(1, chips) for s in (0, 1)]

    for r in range(parts):
        q_arrival(r).wait_recv()
        total = sq_got[r, 0]
        for source in range(1, n_mp):
            total += sq_got[r, source]
        scale = lax.rsqrt(total * (1.0 / (n_mp * width)) + 1e-06)
        scale = jnp.broadcast_to(scale, (8, rows)).T[:, 0:1]
        span = slice(r * rows, (r + 1) * rows)
        for i, source in enumerate(sources):
            if i > 0:
                m_arrival(source, r).wait_recv()
            out[span, columns(source)] = (got[source, span, :].astype(F32) * scale * gain[:, columns(source)]).astype(BF16)

    def sent(ref, sem):
        pltpu.make_async_remote_copy(
            src_ref=ref, dst_ref=ref, send_sem=sem, recv_sem=own_sem,
            device_id={"mp": partner}, device_id_type=MESH).wait_send()

    for step in range(1, chips):
        sent(tokens, y_send.at[step - 1])
        sent(x.at[:, columns(0)], d_send.at[step - 1])
    sent(tokens, p_send)
    sent(sq_out.at[pl.ds(0, chunks - parts)], q_send)
    sent(moved.at[pl.ds(0, seq_rows - own_rows), :], m_send)
    if n_seq > 1:
        pl.when(place < n_seq - 1)(lambda: sent(state_out, s_send))
    if relay:
        pl.when(place == 0)(lambda: sent(hop_out, hop_send))
        pl.when(place == 1)(lambda: sent(hop_in, hop_send))


def in_hbm(a):
    return a if a.size == 1 else pltpu.with_memory_space_constraint(a, pltpu.HBM)


def body(n_mp, n_seq, tokens, w_query, w_key, w_value, w_gate, decay_exponent, forget, norm_gain):
    seq_rows, width = tokens.shape
    features = w_query.shape[0]
    heads = decay_exponent.shape[0]
    own_rows = seq_rows // n_mp
    rows = 256 if own_rows % 256 == 0 else own_rows
    chunks, parts = seq_rows // rows, own_rows // rows
    groups = 2 if heads % 2 == 0 else 1
    hbm = pl.BlockSpec(memory_space=pltpu.HBM)
    transfers = len(token_units(n_mp, n_seq, chunks) or range(chunks))
    dma = pltpu.SemaphoreType.DMA
    chips = n_mp // 2
    return pl.pallas_call(
        functools.partial(kernel, n_mp, n_seq, heads, rows, groups),
        out_shape=pltpu.VMEM((own_rows, features), BF16),
        in_specs=[hbm] * 8,
        out_specs=pl.BlockSpec(memory_space=pltpu.VMEM),
        scratch_shapes=[
            pltpu.VMEM((seq_rows, features), BF16),
            pltpu.VMEM((4, features, width), BF16),
            pltpu.VMEM((1, heads), jnp.int32),
            pltpu.VMEM((heads, seq_rows), F32),
            pltpu.VMEM((1, features), F32),
            pltpu.VMEM((chunks * heads, rows), F32),
            pltpu.VMEM((chunks, heads, rows), F32),
            pltpu.VMEM((chunks, rows, heads), F32),
            pltpu.VMEM((4, 4, rows, width), F32),
            pltpu.VMEM((seq_rows, width), F32),
            pltpu.VMEM((seq_rows, width), BF16),
            pltpu.VMEM((seq_rows, width), F32),
            pltpu.VMEM((seq_rows, width), BF16),
            pltpu.VMEM((n_mp, own_rows, width), BF16),
            pltpu.VMEM((chunks, 1, rows), F32),
            pltpu.VMEM((parts, n_mp, 1, rows), F32),
            pltpu.VMEM((heads, DH, DH), F32),
            pltpu.VMEM((heads, DH, DH), BF16),
            pltpu.VMEM((heads, DH, DH), BF16),
            pltpu.VMEM((heads, DH, DH), BF16),
            pltpu.VMEM((heads, DH, DH), BF16),
            pltpu.VMEM((heads, 128), F32),
            pltpu.VMEM((rows - 64, width), BF16),
            pltpu.VMEM((2, rows - 80, width // groups), BF16),
            dma,
            dma((3,)),
            dma,
            dma((chips - 1,)),
            dma((transfers, chips - 1)),
            dma,
            dma((2,)),
            dma((chips - 1,)),
            dma((transfers, chips - 1)),
            dma,
            dma((groups,)),
            dma,
            dma((n_mp - 1, parts)),
            dma,
            dma((parts,)),
            dma,
            dma((2,)),
            pltpu.SemaphoreType.REGULAR,
        ],
        compiler_params=pltpu.CompilerParams(
            collective_id=0, has_side_effects=True, vmem_limit_bytes=56 * 1024 * 1024
        ),
    )(*(in_hbm(a) for a in (tokens, w_query, w_key, w_value, w_gate, decay_exponent[None, :], forget.T, norm_gain[None, :])))


def solution(mesh):
    placed = (
        P(("dp", "seq"), "mp"),
        P(None, "mp"),
        P(None, "mp"),
        P(None, "mp"),
        P(None, "mp"),
        P("mp"),
        P(("dp", "seq"), "mp"),
        P(),
    )
    return jax.shard_map(
        functools.partial(body, mesh.shape["mp"], mesh.shape["seq"]),
        mesh=mesh,
        in_specs=placed,
        out_specs=P(("dp", "seq", "mp"), None),
        check_vma=False,
    )
```

```python
import functools

import jax
import jax.numpy as jnp
from jax import lax
from jax.experimental import pallas as pl
from jax.experimental.pallas import tpu as pltpu
from jax.sharding import PartitionSpec as P

DH = 128
MESH = pl.DeviceIdType.MESH
F32 = jnp.float32
BF16 = jnp.bfloat16


def contract(a, b, dims):
    return lax.dot_general(a, b, ((dims[0], dims[1]), ((), ())), preferred_element_type=F32)


def kernel(
    n_mp, n_seq, heads, rows, groups,
    tokens, wq, wk, wv, wg, exponent_in, forget_in, gain_in, out,
    x, w, exponent, forget, gain, decays, summed, by_rows, partial, local_out, q_in, gates, moved, got, sq_out, sq_got,
    state, held, enter, state_out, state_got, offset, hop_in, hop_out,
    weight_sem, small_sem, own_sem, y_send, y_recv, p_send, p_recv, d_send, d_recv, s_send, s_recv, m_send, m_recv, q_send, q_recv, hop_send, hop_recv, ready,
):
    me = lax.axis_index("mp")
    place = lax.axis_index("seq")
    chips = n_mp // 2
    chip, core = me // 2, me % 2
    partner = chip * 2 + (1 - core)
    seq_rows, width = tokens.shape
    chunks = seq_rows // rows
    own_rows = seq_rows // n_mp
    parts = own_rows // rows
    head_width = width // heads
    group_heads = heads // groups
    group_width = width // groups
    ahead = partial.shape[0]
    relay = n_seq == 2 and chips == 2
    hop_chunk = 3 if chunks > 4 else chunks - 1
    across = [lax.rem(chip + 1, chips) * 2 + core, lax.rem(chip + 1, chips) * 2 + (1 - core)]

    barrier = pltpu.get_barrier_semaphore()
    greeted = [lax.rem(chip + t, chips) * 2 + core for t in range(1, chips)] + [partner]
    for there in greeted:
        pl.semaphore_signal(barrier, inc=1, device_id={"mp": there}, device_id_type=MESH)

    across_place = [{"seq": 1 - place}] + [{"mp": there, "seq": 1 - place} for there in across]

    if relay:
        @pl.when(place == 0)
        def _():
            for there in across_place:
                pl.semaphore_signal(barrier, inc=1, device_id=there, device_id_type=MESH)
    else:
        @pl.when(place > 0)
        def _():
            pl.semaphore_signal(barrier, inc=1, device_id={"seq": place - 1}, device_id_type=MESH)

        @pl.when(place < n_seq - 1)
        def _():
            pl.semaphore_signal(barrier, inc=1, device_id={"seq": place + 1}, device_id_type=MESH)

    weights = [pltpu.make_async_copy(src, w.at[i], weight_sem) for i, src in enumerate((wk, wv, wq, wg))]
    small = [
        pltpu.make_async_copy(src, dst, small_sem.at[i])
        for i, (src, dst) in enumerate(((exponent_in, exponent), (forget_in, forget), (gain_in, gain)))
    ]

    def relative(source, to):
        return lax.rem(source - to + n_mp, n_mp) - 1

    def columns(block):
        return pl.ds(pl.multiple_of(block * width, width), width)

    def at_rows(c):
        return pl.ds(pl.multiple_of(c * rows, rows), rows)

    def own_copy():
        return pltpu.make_async_copy(tokens, x.at[:, columns(me)], own_sem)

    def far(step):
        return lax.rem(chip + step, chips) * 2 + core

    def back(step):
        return lax.rem(chip + chips - step, chips) * 2 + core

    def back_other(step):
        return lax.rem(chip + chips - step, chips) * 2 + (1 - core)

    def y_copy(c, step):
        return pltpu.make_async_remote_copy(
            src_ref=tokens.at[at_rows(c), :], dst_ref=x.at[at_rows(c), columns(me)],
            send_sem=y_send.at[step - 1], recv_sem=y_recv.at[c, step - 1],
            device_id={"mp": far(step)}, device_id_type=MESH)

    def y_arrival(c, step):
        return pltpu.make_async_remote_copy(
            src_ref=tokens.at[at_rows(c), :], dst_ref=x.at[at_rows(c), columns(back(step))],
            send_sem=y_send.at[step - 1], recv_sem=y_recv.at[c, step - 1],
            device_id={"mp": far(step)}, device_id_type=MESH)

    def at_pair(i):
        return pl.ds(pl.multiple_of(i * 2 * rows, 2 * rows), 2 * rows)

    def p_copy(i):
        return pltpu.make_async_remote_copy(
            src_ref=tokens.at[at_pair(i), :], dst_ref=x.at[at_pair(i), columns(me)],
            send_sem=p_send, recv_sem=p_recv.at[i],
            device_id={"mp": partner}, device_id_type=MESH)

    def p_arrival(i):
        there = x.at[at_pair(i), columns(partner)]
        return pltpu.make_async_remote_copy(
            src_ref=there, dst_ref=there, send_sem=p_send, recv_sem=p_recv.at[i],
            device_id={"mp": partner}, device_id_type=MESH)

    def d_copy(c, step):
        there = x.at[at_rows(c), columns(back(step))]
        return pltpu.make_async_remote_copy(
            src_ref=there, dst_ref=there, send_sem=d_send.at[step - 1], recv_sem=d_recv.at[c, step - 1],
            device_id={"mp": partner}, device_id_type=MESH)

    def d_arrival(c, step):
        there = x.at[at_rows(c), columns(back_other(step))]
        return pltpu.make_async_remote_copy(
            src_ref=there, dst_ref=there, send_sem=d_send.at[step - 1], recv_sem=d_recv.at[c, step - 1],
            device_id={"mp": partner}, device_id_type=MESH)

    kept_rows = rows - hop_in.shape[0]
    hop_span = pl.ds(hop_chunk * rows + kept_rows, rows - kept_rows)

    def y_rest():
        span = pl.ds(hop_chunk * rows, kept_rows)
        return pltpu.make_async_remote_copy(
            src_ref=tokens.at[span, :], dst_ref=x.at[span, columns(me)],
            send_sem=y_send.at[0], recv_sem=y_recv.at[hop_chunk, 0],
            device_id={"mp": across[0]}, device_id_type=MESH)

    def in_hop():
        return pltpu.make_async_remote_copy(
            src_ref=tokens.at[hop_span, :], dst_ref=hop_in,
            send_sem=y_send.at[0], recv_sem=hop_recv.at[0],
            device_id={"mp": across[0], "seq": 1}, device_id_type=MESH)

    def in_next():
        return pltpu.make_async_remote_copy(
            src_ref=hop_in, dst_ref=x.at[hop_span, columns(across[0])],
            send_sem=hop_send, recv_sem=y_recv.at[hop_chunk, 0],
            device_id={"seq": 0}, device_id_type=MESH)

    hop_rows = hop_out.shape[1]

    def out_hop(block, to, i):
        return pltpu.make_async_remote_copy(
            src_ref=moved.at[pl.ds(pl.multiple_of(block * rows, rows), hop_rows), pl.ds(0, group_width)],
            dst_ref=hop_out.at[i], send_sem=m_send, recv_sem=hop_recv.at[i],
            device_id={"mp": to, "seq": 0}, device_id_type=MESH)

    def out_rest(block, to):
        left = rows - hop_rows
        return pltpu.make_async_remote_copy(
            src_ref=moved.at[pl.ds(pl.multiple_of(block * rows + hop_rows, left), left), pl.ds(0, group_width)],
            dst_ref=got.at[me, pl.ds(hop_rows, left), pl.ds(0, group_width)],
            send_sem=m_send, recv_sem=m_recv.at[relative(me, to), 0], device_id={"mp": to}, device_id_type=MESH)

    def out_next(i):
        return pltpu.make_async_remote_copy(
            src_ref=hop_out.at[i], dst_ref=got.at[across[i], pl.ds(0, hop_rows), pl.ds(0, group_width)],
            send_sem=hop_send, recv_sem=m_recv.at[relative(across[i], me), 0],
            device_id={"seq": 1}, device_id_type=MESH)

    for copy in small:
        copy.start()
    own_copy().start()
    for copy in weights:
        copy.start()

    if relay:
        neighbours = place * len(across_place)
    else:
        neighbours = jnp.minimum(place, 1) + jnp.minimum(n_seq - 1 - place, 1)
    pl.semaphore_wait(barrier, len(greeted) + neighbours)

    @pl.loop(0, chunks)
    def _(c):
        for step in range(1, chips):
            if relay:
                whole = jnp.logical_or(place > 0, c != hop_chunk)
                pl.when(whole)(lambda: y_copy(c, step).start())
                pl.when(jnp.logical_not(whole))(lambda: y_rest().start())
            else:
                y_copy(c, step).start()
        pl.when(lax.rem(c, 2) == 0)(lambda: p_copy(c // 2).start())

    if relay:
        @pl.when(place == 1)
        def _():
            for there in across_place:
                pl.semaphore_signal(ready, inc=1, device_id=there, device_id_type=MESH)

    state[...] = jnp.zeros_like(state)
    offset[...] = jnp.zeros_like(offset)
    enter[...] = jnp.zeros_like(enter)

    later = lax.broadcasted_iota(jnp.int32, (rows, rows), 0)
    earlier = lax.broadcasted_iota(jnp.int32, (rows, rows), 1)
    causal = later >= earlier
    summing = (later <= earlier).astype(F32)
    exact = lax.Precision.HIGHEST
    ones = jnp.ones((8, head_width), BF16)

    for copy in small:
        copy.wait()
    spread = jnp.broadcast_to(exponent[...].astype(F32), (heads, heads))
    diagonal = lax.broadcasted_iota(jnp.int32, (heads, heads), 0) == lax.broadcasted_iota(jnp.int32, (heads, heads), 1)
    column = jnp.sum(jnp.where(diagonal, spread, 0.0), axis=1, keepdims=True)
    rate = jnp.log1p(-jnp.exp2(-column))
    for c in range(chunks):
        decays[c * heads : (c + 1) * heads, :] = rate - forget[:, c * rows : (c + 1) * rows]
    every = jnp.dot(decays[...], summing, precision=exact, preferred_element_type=F32)
    turned = every.T
    for c in range(chunks):
        summed[c] = every[c * heads : (c + 1) * heads, :]
        by_rows[c] = turned[:, c * heads : (c + 1) * heads]

    def near(c):
        pl.when(lax.rem(c, 2) == 0)(lambda: p_arrival(c // 2).wait_recv())
        own_side = pl.ds(pl.multiple_of(chip * 2 * width, 2 * width), 2 * width)
        piece = x[at_rows(c), own_side]
        slot = lax.rem(c, ahead)
        for i in range(4):
            partial[slot, i] = jnp.dot(piece, w[i, own_side, :], preferred_element_type=F32)

    if relay:
        @pl.when(place == 0)
        def _():
            pl.semaphore_wait(ready, len(across_place))
            in_hop().start()

    own_copy().wait()
    pltpu.make_async_copy(w, w, weight_sem).wait()
    pl.loop(0, ahead)(near)

    def s_copy(g):
        part = pl.ds(g * group_heads, group_heads)
        return pltpu.make_async_remote_copy(
            src_ref=state_out.at[part], dst_ref=state_got.at[part], send_sem=s_send, recv_sem=s_recv.at[g],
            device_id={"seq": lax.rem(place + 1, n_seq)}, device_id_type=MESH)

    def group_columns(g):
        return pl.ds(g * group_width, group_width)

    def m_copy(block, g):
        to, r = block // parts, lax.rem(block, parts)
        return pltpu.make_async_remote_copy(
            src_ref=moved.at[at_rows(block), group_columns(g)], dst_ref=got.at[me, at_rows(r), group_columns(g)],
            send_sem=m_send, recv_sem=m_recv.at[relative(me, to), r],
            device_id={"mp": to}, device_id_type=MESH)

    def q_copy(block):
        to, r = block // parts, lax.rem(block, parts)
        return pltpu.make_async_remote_copy(
            src_ref=sq_out.at[block], dst_ref=sq_got.at[r, me],
            send_sem=q_send, recv_sem=q_recv.at[r],
            device_id={"mp": to}, device_id_type=MESH)

    def finalize(block, g):
        here = at_rows(block)
        to, r = block // parts, lax.rem(block, parts)
        square = jnp.zeros((rows, head_width), F32)
        for h in range(g * group_heads, (g + 1) * group_heads):
            part = slice(h * head_width, (h + 1) * head_width)
            whole = local_out[here, part] + jnp.dot(q_in[here, part], enter[h], preferred_element_type=F32)
            kept = whole.astype(BF16).astype(F32)
            moved[here, part] = (gates[here, part] * kept).astype(BF16)
            square += kept * kept
        high = square.astype(BF16)
        low = (square - high.astype(F32)).astype(BF16)
        total = (contract(ones, high, ((1,), (1,))) + contract(ones, low, ((1,), (1,))))[0:1, :]
        if g > 0:
            total = total + sq_out[block]
        sq_out[block] = total

        @pl.when(to != me)
        def _():
            if g == groups - 1:
                q_copy(block).start()
            if relay and g == 0:
                detour = jnp.logical_and(jnp.logical_and(place == 1, r == 0), to // 2 != chip)

                @pl.when(detour)
                def _():
                    out_hop(block, to, lax.rem(core + to, 2)).start()
                    out_rest(block, to).start()

                pl.when(jnp.logical_not(detour))(lambda: m_copy(block, g).start())
            else:
                m_copy(block, g).start()

        @pl.when(to == me)
        def _():
            part = slice(g * group_width, (g + 1) * group_width)
            got[me, at_rows(r), part] = moved[here, part]
            if g == groups - 1:
                sq_got[r, me] = total

    far_steps = (n_mp - 2) * parts

    def away(step):
        o = lax.rem(step, n_mp - 2)
        return (lax.rem(chip + o // 2 + 1, chips) * 2 + lax.rem(core + o, 2)) * parts + step // (n_mp - 2)

    def home(step):
        return (chip * 2 + lax.rem(core + 1 + step, 2)) * parts + step // 2

    def enter_state(g):
        part = slice(g * group_heads, (g + 1) * group_heads)
        s_copy(g).wait_recv()
        enter[part] = state_got[part]

    def ready_far(g, low, high):
        @pl.loop(0, far_steps)
        def _(step):
            block = away(lax.rem(step + 2, far_steps) if g == 0 else step)
            pl.when(jnp.logical_and(block >= low, block < high))(lambda: finalize(block, g))

    @pl.loop(0, chunks)
    def _(c):
        here = at_rows(c)
        slot = lax.rem(c, ahead)
        running, by_row = summed[c], by_rows[c]
        last = running[:, rows - 1 :]
        before = offset[...]

        if relay:
            @pl.when(jnp.logical_and(place == 1, c == 1))
            def _():
                in_hop().wait_recv()
                in_next().start()

            @pl.when(jnp.logical_and(place == 1, c == chunks - 1))
            def _():
                ready_far(0, chunks - 2, chunks - 1)
                for g in range(1, groups):
                    enter_state(g)
                    ready_far(g, 0, chunks - 1)

        for step in range(1, chips):
            y_arrival(c, step).wait_recv()
            d_copy(c, step).start()
        for step in range(1, chips):
            piece = x[here, columns(back(step))]
            for i in range(4):
                partial[slot, i] += jnp.dot(piece, w[i, columns(back(step)), :], preferred_element_type=F32)

        @pl.when(jnp.logical_and(place == 0, c > 0))
        def _():
            for g in range(groups):
                finalize(c - 1, g)

        for step in range(1, chips):
            d_arrival(c, step).wait_recv()

        if relay:
            @pl.when(jnp.logical_and(place == 1, c == chunks - 2))
            def _():
                enter_state(0)
                ready_far(0, 0, chunks - 2)

        def project(i):
            total = partial[slot, i]
            for step in range(1, chips):
                total += jnp.dot(
                    x[here, columns(back_other(step))], w[i, columns(back_other(step)), :],
                    preferred_element_type=F32)
            return total

        key = (project(0) * DH ** (-0.5)).astype(BF16)
        value = project(1).astype(BF16)
        for h in range(heads):
            part = slice(h * head_width, (h + 1) * head_width)
            k, v = key[:, part], value[:, part]
            end = last[h : h + 1, :]
            grown = state[h]
            held[h] = grown.astype(BF16)
            faded = (k.astype(F32) * jnp.exp(end - by_row[:, h : h + 1])).astype(BF16)
            state[h] = jnp.exp(end) * grown + contract(faded, v, ((0,), (0,)))

        @pl.when(jnp.logical_and(place == 0, c == chunks - 1))
        def _():
            state_out[...] = state[...].astype(BF16)
            if n_seq > 1:
                for g in range(groups):
                    s_copy(g).start()

        query = project(2).astype(BF16)
        for h in range(heads):
            part = slice(h * head_width, (h + 1) * head_width)
            q, k, v = query[:, part], key[:, part], value[:, part]
            col = by_row[:, h : h + 1]
            mask = jnp.exp(jnp.where(causal, col - running[h : h + 1, :], -1e30))
            scores = (contract(q, k, ((1,), (1,))) * mask).astype(BF16)
            qf = q.astype(F32)
            carried = jnp.dot((qf * jnp.exp(col)).astype(BF16), held[h], preferred_element_type=F32)
            local_out[here, part] = jnp.dot(scores, v, preferred_element_type=F32) + carried
            q_in[here, part] = (qf * jnp.exp(col + before[h : h + 1, 0:1])).astype(BF16)
        offset[...] = before + last
        gate = project(3).astype(BF16).astype(F32)
        gates[here, :] = gate / (1.0 + jnp.exp(-gate))

        pl.when(c < chunks - ahead)(lambda: near(c + ahead))

    @pl.when(place == 0)
    def _():
        for g in range(groups):
            finalize(chunks - 1, g)

    if n_seq > 1:
        @pl.when(place > 0)
        def _():
            for g in range(groups):
                if relay:
                    pl.when((chunks - 1) // parts // 2 != chip)(lambda: finalize(chunks - 1, g))
                    continue
                enter_state(g)
                if n_seq > 2:
                    @pl.when(place < n_seq - 1)
                    def _():
                        for h in range(g * group_heads, (g + 1) * group_heads):
                            total = jnp.exp(offset[h : h + 1, 0:1])
                            state_out[h] = (total * enter[h].astype(F32) + state[h]).astype(BF16)
                        s_copy(g).start()

                pl.loop(0, far_steps)(lambda step: finalize(away(step), g))

            @pl.loop(0, 2 * parts)
            def _(step):
                for g in range(groups):
                    finalize(home(step), g)

    if relay:
        @pl.when(place == 0)
        def _():
            for i in range(2):
                out_hop(0, across[i], i).wait_recv()
                out_next(i).start()

    def m_arrival(source, r):
        there = got.at[source, at_rows(r), :]
        return pltpu.make_async_remote_copy(
            src_ref=there, dst_ref=there, send_sem=m_send, recv_sem=m_recv.at[relative(source, me), r],
            device_id={"mp": partner}, device_id_type=MESH)

    def q_arrival(r):
        there = sq_got.at[r, pl.ds(0, n_mp - 1)]
        return pltpu.make_async_remote_copy(
            src_ref=there, dst_ref=there, send_sem=q_send, recv_sem=q_recv.at[r],
            device_id={"mp": partner}, device_id_type=MESH)

    sources = [me, partner] + [lax.rem(chip + t, chips) * 2 + lax.rem(core + s, 2) for t in range(1, chips) for s in (0, 1)]

    for r in range(parts):
        q_arrival(r).wait_recv()
        total = sq_got[r, 0]
        for source in range(1, n_mp):
            total += sq_got[r, source]
        scale = lax.rsqrt(total * (1.0 / (n_mp * width)) + 1e-06)
        scale = jnp.broadcast_to(scale, (8, rows)).T[:, 0:1]
        span = slice(r * rows, (r + 1) * rows)
        for i, source in enumerate(sources):
            if i > 0:
                m_arrival(source, r).wait_recv()
            out[span, columns(source)] = (got[source, span, :].astype(F32) * scale * gain[:, columns(source)]).astype(BF16)

    def sent(ref, sem):
        pltpu.make_async_remote_copy(
            src_ref=ref, dst_ref=ref, send_sem=sem, recv_sem=own_sem,
            device_id={"mp": partner}, device_id_type=MESH).wait_send()

    for step in range(1, chips):
        sent(tokens, y_send.at[step - 1])
        sent(x.at[:, columns(0)], d_send.at[step - 1])
    sent(tokens, p_send)
    sent(sq_out.at[pl.ds(0, chunks - parts)], q_send)
    sent(moved.at[pl.ds(0, seq_rows - own_rows), :], m_send)
    if n_seq > 1:
        pl.when(place < n_seq - 1)(lambda: sent(state_out, s_send))
    if relay:
        pl.when(place == 0)(lambda: sent(hop_out, hop_send))
        pl.when(place == 1)(lambda: sent(hop_in, hop_send))


def in_hbm(a):
    return a if a.size == 1 else pltpu.with_memory_space_constraint(a, pltpu.HBM)


def body(n_mp, n_seq, tokens, w_query, w_key, w_value, w_gate, decay_exponent, forget, norm_gain):
    seq_rows, width = tokens.shape
    features = w_query.shape[0]
    heads = decay_exponent.shape[0]
    own_rows = seq_rows // n_mp
    rows = 256 if own_rows % 256 == 0 else own_rows
    chunks, parts = seq_rows // rows, own_rows // rows
    groups = 2 if heads % 2 == 0 else 1
    hbm = pl.BlockSpec(memory_space=pltpu.HBM)
    dma = pltpu.SemaphoreType.DMA
    chips = n_mp // 2
    return pl.pallas_call(
        functools.partial(kernel, n_mp, n_seq, heads, rows, groups),
        out_shape=pltpu.VMEM((own_rows, features), BF16),
        in_specs=[hbm] * 8,
        out_specs=pl.BlockSpec(memory_space=pltpu.VMEM),
        scratch_shapes=[
            pltpu.VMEM((seq_rows, features), BF16),
            pltpu.VMEM((4, features, width), BF16),
            pltpu.VMEM((1, heads), jnp.int32),
            pltpu.VMEM((heads, seq_rows), F32),
            pltpu.VMEM((1, features), F32),
            pltpu.VMEM((chunks * heads, rows), F32),
            pltpu.VMEM((chunks, heads, rows), F32),
            pltpu.VMEM((chunks, rows, heads), F32),
            pltpu.VMEM((4, 4, rows, width), F32),
            pltpu.VMEM((seq_rows, width), F32),
            pltpu.VMEM((seq_rows, width), BF16),
            pltpu.VMEM((seq_rows, width), F32),
            pltpu.VMEM((seq_rows, width), BF16),
            pltpu.VMEM((n_mp, own_rows, width), BF16),
            pltpu.VMEM((chunks, 1, rows), F32),
            pltpu.VMEM((parts, n_mp, 1, rows), F32),
            pltpu.VMEM((heads, DH, DH), F32),
            pltpu.VMEM((heads, DH, DH), BF16),
            pltpu.VMEM((heads, DH, DH), BF16),
            pltpu.VMEM((heads, DH, DH), BF16),
            pltpu.VMEM((heads, DH, DH), BF16),
            pltpu.VMEM((heads, 128), F32),
            pltpu.VMEM((rows - 64, width), BF16),
            pltpu.VMEM((2, rows - 64, width // groups), BF16),
            dma,
            dma((3,)),
            dma,
            dma((chips - 1,)),
            dma((chunks, chips - 1)),
            dma,
            dma((chunks // 2,)),
            dma((chips - 1,)),
            dma((chunks, chips - 1)),
            dma,
            dma((groups,)),
            dma,
            dma((n_mp - 1, parts)),
            dma,
            dma((parts,)),
            dma,
            dma((2,)),
            pltpu.SemaphoreType.REGULAR,
        ],
        compiler_params=pltpu.CompilerParams(
            collective_id=0, has_side_effects=True, vmem_limit_bytes=56 * 1024 * 1024
        ),
    )(*(in_hbm(a) for a in (tokens, w_query, w_key, w_value, w_gate, decay_exponent[None, :], forget.T, norm_gain[None, :])))


def solution(mesh):
    placed = (
        P(("dp", "seq"), "mp"),
        P(None, "mp"),
        P(None, "mp"),
        P(None, "mp"),
        P(None, "mp"),
        P("mp"),
        P(("dp", "seq"), "mp"),
        P(),
    )
    return jax.shard_map(
        functools.partial(body, mesh.shape["mp"], mesh.shape["seq"]),
        mesh=mesh,
        in_specs=placed,
        out_specs=P(("dp", "seq", "mp"), None),
        check_vma=False,
    )
```
